128 devices in a mesh: depth: 16 (over y, x), screen: 8 (over z, core).
Axes of the slice: x: 4, y: 4, z: 4, core: 2. Of those that a mesh axis runs over, the one named last changes fastest.
Arguments:
- block_tile: int32 [16, 16384], P('depth', 'screen'), may hold values from 0 to 511
- block_count: int32 [16, 8], P('depth', 'screen'), may hold values from 256 to 2048, as said below
- slab_rank: int32 [16], replicated, may hold values from 0 to 15, each once
- corner: int32 [2, 16, 16384, 128], P(None, 'depth', 'screen'), may hold values from 0 to 16
- offset: float32 [2, 16, 16384, 128], P(None, 'depth', 'screen'), may hold values from 0.25 to 0.75
- radius: float32 [16, 16384, 128], P('depth', 'screen'), may hold values from 3 to 8
- emission: float32 [3, 16, 16384, 128], P(None, 'depth', 'screen'), may hold values from 0.002 to 0.02
- extinction: float32 [16, 16384, 128], P('depth', 'screen'), may hold values from 0.001 to 0.01
Outputs:
- image_tiles: float32 [512, 32, 128], P(('depth', 'screen'))
The draws below stay inside these ranges and needn't reach their ends.
Inputs may be any that keep to these rules, and one draw needn't show every extreme that they name: The live slots of a device are its first block_count slots; one device of every draw has all 2048 slots live. `block_tile`: a block holds particles of one tile. `corner`: a footprint box lies inside its tile. `slab_rank`: each slab once.
All inputs are finite; a program needn't handle non-finite values.
Results may differ from the reference program's by a relative error of at most 0.0003.
Values sent between devices are 32-bit elements; how exact they have to be, the bound alone decides.
A program may use at most 128 MiB of HBM per device.

```python
import math
import jax
import jax.numpy as jnp
import numpy as np
from jax import lax

TS = 32
FOOT = 16
PB = 128
BLK_DEV = 2048
TILES = 512
N_DEPTH = 16
N_SCREEN = 8


def draw_block_count(key, part):
    counts = jax.random.randint(key, (N_DEPTH, N_SCREEN), max(1, BLK_DEV // 8), BLK_DEV // 2 + 1)
    fullest = jax.random.randint(jax.random.fold_in(key, 7), (), 0, N_DEPTH * N_SCREEN)
    flattened = jnp.where(jnp.arange(N_DEPTH * N_SCREEN) == fullest, BLK_DEV, counts.reshape(-1))
    return flattened.reshape(N_DEPTH, N_SCREEN).astype(jnp.int32)


def place_ends(values, rng, low, high):
    shape = values.shape
    index_at = [jax.random.randint(jax.random.fold_in(rng, axis), (), 0, shape[axis]) for axis in range(len(shape))]
    values = values.at[tuple(index_at)].set(low)
    longest = shape.index(max(shape))
    index_at[longest] = (index_at[longest] + 1) % shape[longest]
    return values.at[tuple(index_at)].set(high)


def block_levels(rng, shape, cuts, low, high):
    factor_of = 1.0
    for axis_at, parts in cuts:
        steps = jax.random.uniform(jax.random.fold_in(jax.random.fold_in(rng, 6), axis_at), (parts,), jnp.float32, low / len(cuts), high / len(cuts))
        factor_of = factor_of * jnp.repeat(jnp.exp(steps), shape[axis_at] // parts).reshape((-1,) + (1,) * (len(shape) - 1 - axis_at))
    return factor_of


def rank_table(count, lean):
    loads = [(1 << 20) // math.isqrt(rank ** lean) + 1 for rank in range(1, count + 1)]
    scale = 1 + sum(loads) // (1 << 30)
    return np.cumsum(np.array([max(1, weight // scale) for weight in loads]))


def ranked(rng, dims, amount, slope):
    table = rank_table(amount, slope)
    pick = jax.random.randint(jax.random.fold_in(rng, 1), dims, 0, int(table[amount - 1]))
    grade = jnp.searchsorted(jnp.asarray(table, jnp.int32), pick, side="right")
    return jax.random.permutation(jax.random.fold_in(rng, 2), amount)[grade].astype(jnp.int32)


def setup_inputs(seed: int = 0) -> dict:
    seeds = jax.random.split(jax.random.key(seed), 9)
    return {
        "block_tile": place_ends(ranked(seeds[0], (N_DEPTH, N_SCREEN * BLK_DEV), TILES, 1), jax.random.fold_in(seeds[0], 3), 0, TILES - 1).astype(jnp.int32),
        "block_count": draw_block_count(jax.random.fold_in(seeds[8], 71), 0),
        "slab_rank": jax.random.permutation(seeds[2], N_DEPTH).astype(jnp.int32),
        "corner": place_ends(jax.random.randint(seeds[3], (2, N_DEPTH, N_SCREEN * BLK_DEV, PB), 0, TS - FOOT + 1), jax.random.fold_in(seeds[3], 1), 0, TS - FOOT).astype(jnp.int32),
        "offset": jnp.clip(0.25 + 0.5 * jax.random.uniform(seeds[4], (2, N_DEPTH, N_SCREEN * BLK_DEV, PB), jnp.float32) ** block_levels(seeds[4], (2, N_DEPTH, N_SCREEN * BLK_DEV, PB), ((1, 16), (2, 8)), -0.2, 0.2), 0.25, 0.75),
        "radius": jnp.clip(3.0 + 5.0 * jax.random.uniform(seeds[5], (N_DEPTH, N_SCREEN * BLK_DEV, PB), jnp.float32) ** block_levels(seeds[5], (N_DEPTH, N_SCREEN * BLK_DEV, PB), ((0, 16), (1, 8)), -0.2, 0.2), 3.0, 8.0),
        "emission": jnp.clip(jnp.exp(math.log(0.02) - 2.30258502 * jax.random.uniform(seeds[6], (3, N_DEPTH, N_SCREEN * BLK_DEV, PB), jnp.float32) ** block_levels(seeds[6], (3, N_DEPTH, N_SCREEN * BLK_DEV, PB), ((1, 16), (2, 8)), -0.2, 0.2)), 0.002, 0.02),
        "extinction": jnp.clip(jnp.exp(math.log(0.01) - 2.30258502 * jax.random.uniform(seeds[7], (N_DEPTH, N_SCREEN * BLK_DEV, PB), jnp.float32) ** block_levels(seeds[7], (N_DEPTH, N_SCREEN * BLK_DEV, PB), ((0, 16), (1, 8)), -0.2, 0.2)), 0.001, 0.01),
    }


def axis_weights(corner, offset, radius, tile_side, foot):
    pixel_index = jnp.arange(tile_side, dtype=jnp.int32)
    pixel_centre = pixel_index.astype(jnp.float32) + 0.5
    centres = corner.astype(jnp.float32) + foot * offset
    scaled = (pixel_centre - centres[..., None]) / radius[..., None]
    bump_shape = jnp.maximum(1.0 - scaled * scaled, 0.0)
    inside = (pixel_index >= corner[..., None]) & (pixel_index < corner[..., None] + foot)
    return jnp.where(inside, bump_shape * bump_shape, 0.0)


def deposit(corner, offset, radius, emission, extinction, block_live, tile_side, foot):
    across = axis_weights(corner[0], offset[0], radius, tile_side, foot)
    down_weights = axis_weights(corner[1], offset[1], radius, tile_side, foot)
    fields = jnp.concatenate([emission, extinction[None]], 0) * block_live[None, :, None]
    spread = fields[..., None] * across[None]
    deposit_out = jnp.einsum('gpy,cgpx->gycx', down_weights, spread, precision=lax.Precision.HIGHEST)
    return deposit_out.reshape(deposit_out.shape[0], tile_side, 4 * tile_side)


def composite(stacked, slab_rank):
    slab_num, tile_num, tile_side, row_width = stacked.shape
    pieces = stacked.reshape(slab_num, tile_num, tile_side, 4, row_width // 4)
    glow_part = pieces[:, :, :, :3, :]
    optical = pieces[:, :, :, 3:, :]
    before = (slab_rank[None, :] < slab_rank[:, None]).astype(jnp.float32)
    prior_depth = jnp.einsum('jk,ktyax->jtyax', before, optical, precision=lax.Precision.HIGHEST)
    lighting = jnp.sum(jnp.exp(-prior_depth) * glow_part * jnp.exp(-0.5 * optical), axis=0)
    coverage = 1.0 - jnp.exp(-jnp.sum(optical, axis=0))
    return jnp.concatenate([lighting, coverage], axis=2).reshape(tile_num, tile_side, row_width)


def reference(block_tile, block_count, slab_rank, corner, offset, radius, emission, extinction):
    group_size = min(256, BLK_DEV)
    rounds = BLK_DEV // group_size
    tile_ids = block_tile.reshape(N_DEPTH, N_SCREEN, rounds, group_size)
    corners = jnp.moveaxis(corner.reshape(2, N_DEPTH, N_SCREEN, rounds, group_size, PB), 0, 3)
    offsets = jnp.moveaxis(offset.reshape(2, N_DEPTH, N_SCREEN, rounds, group_size, PB), 0, 3)
    radii = radius.reshape(N_DEPTH, N_SCREEN, rounds, group_size, PB)
    glows = jnp.moveaxis(emission.reshape(3, N_DEPTH, N_SCREEN, rounds, group_size, PB), 0, 3)
    rates = extinction.reshape(N_DEPTH, N_SCREEN, rounds, group_size, PB)

    def one_device(running, device_inputs):
        ids_dev, live_count, corner_dev, offset_dev, radius_dev, glow_dev, rate_dev = device_inputs
        slot_live = (jnp.arange(BLK_DEV, dtype=jnp.int32) < live_count).astype(jnp.float32)
        slot_live = slot_live.reshape(rounds, group_size)

        def one_round(tile_sums, round_inputs):
            ids_now, live_now, corner_now, offset_now, radius_now, glow_now, rate_now = round_inputs
            deposit_out = deposit(corner_now, offset_now, radius_now, glow_now, rate_now, live_now, TS, FOOT)
            return tile_sums.at[ids_now].add(deposit_out), None

        tile_sums, unused = lax.scan(one_round, jnp.zeros((TILES, TS, 4 * TS), jnp.float32),
                                     (ids_dev, slot_live, corner_dev, offset_dev, radius_dev, glow_dev, rate_dev))
        return running + tile_sums, None

    def one_slab(slab_inputs):
        running, unused = lax.scan(one_device, jnp.zeros((TILES, TS, 4 * TS), jnp.float32), slab_inputs)
        return running

    slab_stack = lax.map(one_slab, (tile_ids, block_count, corners, offsets, radii, glows, rates))
    return composite(slab_stack, slab_rank)
```

```python
import jax
import jax.numpy as jnp
from jax import lax
from jax.experimental import pallas as pl
from jax.experimental.pallas import tpu as pltpu
from jax.sharding import Mesh
from jax.sharding import PartitionSpec as P

TS = 32
FOOT = 16
TILE_DEV = 4
SCREEN = ("screen_0", "screen_1")
DEPTH_SCREEN = ("depth", "screen_0", "screen_1")


def sum_in_order(pieces, axes, turns):
    inside = pieces.shape[1:]
    pieces = pieces.reshape(*(lax.axis_size(a) for a in axes), *inside)
    pieces = jnp.moveaxis(pieces, turns, range(len(axes))).reshape(-1, *inside)
    for k in turns:
        pieces = lax.psum_scatter(pieces, axes[k], scatter_dimension=0, tiled=True)
    return pieces[0]


def cut_along(shard, dim, devices):
    before, after = (shard.shape[:dim], shard.shape[dim + 1 :])
    return jnp.moveaxis(shard.reshape(*before, devices, -1, *after), dim, 0)


def summed_rows(shard, axes, turns, dim):
    devices = lax.axis_size(axes)
    return sum_in_order(cut_along(shard, dim, devices), axes, turns)


BLK = 128
UNR = 32

def deposit_kernel(tile_ref, count_ref, corner_ref, offset_ref, radius_ref, emission_ref, extinction_ref, out_ref, pre_ref):
    step = pl.program_id(0)
    count = count_ref[0, 0]

    @pl.when(step == 0)
    def _():
        def zero(t, c):
            out_ref[t] = jnp.zeros(out_ref.shape[1:], jnp.float32)
            return c
        lax.fori_loop(0, out_ref.shape[0], zero, 0, unroll=8)

    first = step * BLK

    @pl.when(first < count)
    def _():
        slot = first + lax.broadcasted_iota(jnp.int32, (BLK, 128), 0)
        live = slot < count
        radius = radius_ref[0]
        h2 = radius * radius
        h4 = h2 * h2
        scale = jnp.where(live, 1.0 / (h4 * h4), 0.0)
        for k in range(2):
            edge = corner_ref[k, 0].astype(jnp.float32)
            pre_ref[2 * k] = edge
            pre_ref[2 * k + 1] = edge + 16.0 * offset_ref[k, 0] - 0.5
        pre_ref[4] = h2
        for c in range(3):
            pre_ref[5 + c] = emission_ref[c, 0] * scale
        pre_ref[8] = extinction_ref[0] * scale

        rows = lax.broadcasted_iota(jnp.int32, (16, 128), 0).astype(jnp.float32)
        rows16 = rows.astype(jnp.bfloat16)
        zero16 = jnp.zeros((16, 128), jnp.bfloat16)

        def split(w):
            high = w.astype(jnp.bfloat16)
            low = (w - high.astype(jnp.float32)).astype(jnp.bfloat16)
            return high, low

        def one_group(g, c):
            outs = []
            for u in range(UNR):
                j = g * UNR + u
                def row(a):
                    return jnp.broadcast_to(pre_ref[a, pl.ds(j, 1), :], (16, 128))
                h2r = row(4)
                def bump(k):
                    edge = row(2 * k)
                    mask16 = rows16 < edge.astype(jnp.bfloat16)
                    at = jnp.where(rows < edge, rows + 16.0, rows)
                    s = at - row(2 * k + 1)
                    v = jnp.maximum(h2r - s * s, 0.0)
                    return v * v, mask16
                wx, mx = bump(0)
                wy, my = bump(1)
                def spread(w16, m):
                    return [jnp.where(m, zero16, w16), jnp.where(m, w16, zero16)]
                yh, yl = split(wy)
                lhs = jnp.concatenate(spread(yh, my) + spread(yl, my), 0)
                lhs = jnp.concatenate([lhs, lhs], 1)
                hi, lo = [], []
                for ch in range(4):
                    a, b = split(row(5 + ch) * wx)
                    hi += spread(a, mx)
                    lo += spread(b, mx)
                rhs = jnp.concatenate([jnp.concatenate(hi, 0), jnp.concatenate(lo, 0)], 1)
                outs.append(lax.dot_general(lhs, rhs, (((1,), (1,)), ((), ())), preferred_element_type=jnp.float32))
            for u in range(UNR):
                t = tile_ref[0, first + g * UNR + u]
                out_ref[t] += outs[u][:32] + outs[u][32:]
            return c

        groups = lax.div(jnp.minimum(count - first, BLK) + (UNR - 1), UNR)
        lax.fori_loop(0, groups, one_group, 0)


def deposit_all(block_tile, block_count, corner, offset, radius, emission, extinction, tiles=512):
    slots = block_tile.shape[1]
    steps = slots // BLK
    def last(i, tile, count):
        return jnp.minimum(i, lax.div(count[0, 0] - 1, BLK))
    def m4(n):
        return pl.BlockSpec((n, 1, BLK, 128), lambda i, t, c: (0, 0, last(i, t, c), 0))
    def m3():
        return pl.BlockSpec((1, BLK, 128), lambda i, t, c: (0, last(i, t, c), 0))
    return pl.pallas_call(
        deposit_kernel,
        out_shape=jax.ShapeDtypeStruct((tiles, 32, 128), jnp.float32),
        grid_spec=pltpu.PrefetchScalarGridSpec(
            num_scalar_prefetch=2, grid=(steps,),
            in_specs=[m4(2), m4(2), m3(), m4(3), m3()],
            out_specs=pl.BlockSpec((tiles, 32, 128), lambda i, t, c: (0, 0, 0)),
            scratch_shapes=[pltpu.VMEM((9, BLK, 128), jnp.float32)],
        ),
        compiler_params=pltpu.CompilerParams(dimension_semantics=("arbitrary",)),
        name="deposit",
    )(block_tile, block_count, corner, offset, radius, emission, extinction)


def composite(stacked, slab_rank):
    slab_num, tile_num, tile_side, row_width = stacked.shape
    pieces = stacked.reshape(slab_num, tile_num, tile_side, 4, row_width // 4)
    glow_part = pieces[:, :, :, :3, :]
    optical = pieces[:, :, :, 3:, :]
    before = (slab_rank[None, :] < slab_rank[:, None]).astype(jnp.float32)
    prior_depth = jnp.einsum("jk,ktyax->jtyax", before, optical, precision=lax.Precision.HIGHEST)
    lighting = jnp.sum(jnp.exp(-prior_depth) * glow_part * jnp.exp(-0.5 * optical), axis=0)
    coverage = 1.0 - jnp.exp(-jnp.sum(optical, axis=0))
    return jnp.concatenate([lighting, coverage], axis=2).reshape(tile_num, tile_side, row_width)


def shards(block_tile, block_count, slab_rank, corner, offset, radius, emission, extinction):
    depth_size = lax.axis_size("depth")
    screen_size = lax.axis_size(SCREEN)
    partial_value = deposit_all(
        block_tile, block_count, corner, offset, radius, emission, extinction,
        TILE_DEV * depth_size * screen_size,
    )
    shaped = partial_value.reshape(depth_size, screen_size * TILE_DEV, TS, 4 * TS)
    owned = summed_rows(shaped, SCREEN, (1, 0), 1)
    return composite(
        lax.all_to_all(owned, "depth", split_axis=0, concat_axis=0, tiled=True), slab_rank
    )


def solution(mesh):
    torus = Mesh(mesh.devices.reshape(mesh.shape["depth"], 4, 2), ("depth", "screen_0", "screen_1"))
    placed = (
        P("depth", SCREEN),
        P("depth", SCREEN),
        P(),
        P(None, "depth", SCREEN, None),
        P(None, "depth", SCREEN, None),
        P("depth", SCREEN, None),
        P(None, "depth", SCREEN, None),
        P("depth", SCREEN, None),
    )
    return jax.shard_map(
        shards, mesh=torus, in_specs=placed, out_specs=P(DEPTH_SCREEN, None, None), check_vma=False
    )
```

```python
import jax
import jax.numpy as jnp
from jax import lax
from jax.experimental import pallas as pl
from jax.experimental.pallas import tpu as pltpu
from jax.sharding import Mesh
from jax.sharding import PartitionSpec as P

SCREEN = ("screen_0", "screen_1")
DEPTH_SCREEN = ("depth", "screen_0", "screen_1")
BLK = 128
UNR = 32

def deposit_kernel(tile_ref, count_ref, corner_ref, offset_ref, radius_ref, emission_ref, extinction_ref, out_ref, pre_ref):
    step = pl.program_id(0)
    count = count_ref[0, 0]

    @pl.when(step == 0)
    def _():
        def zero(t, c):
            out_ref[t] = jnp.zeros(out_ref.shape[1:], jnp.float32)
            return c
        lax.fori_loop(0, out_ref.shape[0], zero, 0, unroll=8)

    first = step * BLK

    @pl.when(first < count)
    def _():
        slot = first + lax.broadcasted_iota(jnp.int32, (BLK, 128), 0)
        live = slot < count
        radius = radius_ref[0]
        h2 = radius * radius
        h4 = h2 * h2
        scale = jnp.where(live, 1.0 / (h4 * h4), 0.0)
        for k in range(2):
            edge = corner_ref[k, 0].astype(jnp.float32)
            pre_ref[2 * k] = edge
            pre_ref[2 * k + 1] = edge + 16.0 * offset_ref[k, 0] - 0.5
        pre_ref[4] = h2
        for c in range(3):
            pre_ref[5 + c] = emission_ref[c, 0] * scale
        pre_ref[8] = extinction_ref[0] * scale

        rows = lax.broadcasted_iota(jnp.int32, (16, 128), 0).astype(jnp.float32)
        rows16 = rows.astype(jnp.bfloat16)
        zero16 = jnp.zeros((16, 128), jnp.bfloat16)

        def split(w):
            high = w.astype(jnp.bfloat16)
            low = (w - high.astype(jnp.float32)).astype(jnp.bfloat16)
            return high, low

        def one_group(g, c):
            outs = []
            for u in range(UNR):
                j = g * UNR + u
                def row(a):
                    return jnp.broadcast_to(pre_ref[a, pl.ds(j, 1), :], (16, 128))
                h2r = row(4)
                def bump(k):
                    edge = row(2 * k)
                    mask16 = rows16 < edge.astype(jnp.bfloat16)
                    at = jnp.where(rows < edge, rows + 16.0, rows)
                    s = at - row(2 * k + 1)
                    v = jnp.maximum(h2r - s * s, 0.0)
                    return v * v, mask16
                wx, mx = bump(0)
                wy, my = bump(1)
                def spread(w16, m):
                    return [jnp.where(m, zero16, w16), jnp.where(m, w16, zero16)]
                yh, yl = split(wy)
                lhs = jnp.concatenate(spread(yh, my) + spread(yl, my), 0)
                lhs = jnp.concatenate([lhs, lhs], 1)
                hi, lo = [], []
                for ch in range(4):
                    a, b = split(row(5 + ch) * wx)
                    hi += spread(a, mx)
                    lo += spread(b, mx)
                rhs = jnp.concatenate([jnp.concatenate(hi, 0), jnp.concatenate(lo, 0)], 1)
                outs.append(lax.dot_general(lhs, rhs, (((1,), (1,)), ((), ())), preferred_element_type=jnp.float32))
            for u in range(UNR):
                t = tile_ref[0, first + g * UNR + u]
                out_ref[t] += outs[u][:32] + outs[u][32:]
            return c

        groups = lax.div(jnp.minimum(count - first, BLK) + (UNR - 1), UNR)
        lax.fori_loop(0, groups, one_group, 0)


def deposit_all(block_tile, block_count, corner, offset, radius, emission, extinction, tiles=512):
    slots = block_tile.shape[1]
    steps = slots // BLK
    def last(i, tile, count):
        return jnp.minimum(i, lax.div(count[0, 0] - 1, BLK))
    def m4(n):
        return pl.BlockSpec((n, 1, BLK, 128), lambda i, t, c: (0, 0, last(i, t, c), 0))
    def m3():
        return pl.BlockSpec((1, BLK, 128), lambda i, t, c: (0, last(i, t, c), 0))
    return pl.pallas_call(
        deposit_kernel,
        out_shape=jax.ShapeDtypeStruct((tiles, 32, 128), jnp.float32),
        grid_spec=pltpu.PrefetchScalarGridSpec(
            num_scalar_prefetch=2, grid=(steps,),
            in_specs=[m4(2), m4(2), m3(), m4(3), m3()],
            out_specs=pl.BlockSpec((tiles, 32, 128), lambda i, t, c: (0, 0, 0)),
            scratch_shapes=[pltpu.VMEM((9, BLK, 128), jnp.float32)],
        ),
        compiler_params=pltpu.CompilerParams(dimension_semantics=("arbitrary",)),
        name="deposit",
    )(block_tile, block_count, corner, offset, radius, emission, extinction)


MESH_ID = pl.DeviceIdType.MESH


def exchange_kernel(order_ref, partial_ref, image_ref, mine, pair, from_up, from_down, via_up, via_down, stack,
                    local_sem, pair_send, pair_recv, far_send, far_recv, near_send, near_recv, sum_send, sum_recv,
                    stack_send, stack_recv):
    d = lax.axis_index("depth")
    z = lax.axis_index("screen_0")
    core = lax.axis_index("screen_1")
    mate = 1 - core
    y, x = lax.div(d, 4), lax.rem(d, 4)
    z_up, z_down, z_far = lax.rem(z + 1, 4), lax.rem(z + 3, 4), lax.rem(z + 2, 4)
    turns = (2, 1, 3, 0)
    others = [(ry, rx) for ry in turns for rx in (2, 1, 3, 0) if (ry, rx) != (0, 0)]

    def away(ry, rx):
        return lax.rem(y + ry, 4) * 4 + lax.rem(x + rx, 4)

    def row(ry):
        return lax.rem(y + ry, 4) * 4

    barrier = pltpu.get_barrier_semaphore()
    pl.semaphore_signal(barrier, inc=1, device_id={"screen_1": mate}, device_id_type=MESH_ID)
    pl.semaphore_signal(barrier, inc=1, device_id={"screen_0": z_up}, device_id_type=MESH_ID)
    pl.semaphore_signal(barrier, inc=1, device_id={"screen_0": z_down}, device_id_type=MESH_ID)
    for ry, rx in others:
        pl.semaphore_signal(barrier, inc=1, device_id={"depth": away(ry, rx)}, device_id_type=MESH_ID)

    places = (z_far, z_up, z_down, z)

    def local_copy(p, g):
        rows = pl.ds(row(g), 4)
        return pltpu.make_async_copy(
            partial_ref.at[rows, places[p], core], mine.at[rows, places[p]], local_sem.at[p, g])

    def pair_copy(p, g):
        rows = pl.ds(row(g), 4)
        return pltpu.make_async_remote_copy(
            partial_ref.at[rows, places[p], mate], pair.at[rows, places[p]],
            pair_send.at[p, g], pair_recv.at[p, g], device_id={"screen_1": mate}, device_id_type=MESH_ID)

    def line_copy(g, half, place, goal, to_up, send, recv):
        rows = pl.ds(row(g) + 2 * half, 2)
        return pltpu.make_async_remote_copy(
            mine.at[rows, place], goal.at[rows], send.at[to_up, g], recv.at[to_up, g],
            device_id={"screen_0": z_up if to_up else z_down}, device_id_type=MESH_ID)

    def far_copy(g, to_up):
        return line_copy(g, 1 - to_up, z_far, via_up if to_up else via_down, to_up, far_send, far_recv)

    def near_copy(g, to_up):
        return line_copy(g, to_up, z_up if to_up else z_down, from_up if to_up else from_down, to_up,
                         near_send, near_recv)

    def sum_copy(g, to_up):
        return line_copy(g, 1 - to_up, z_up if to_up else z_down, from_up if to_up else from_down, to_up,
                         sum_send, sum_recv)

    def stack_copy(ry, rx):
        to = away(ry, rx)
        return pltpu.make_async_remote_copy(
            mine.at[to, z], stack.at[d], stack_send.at[ry, rx], stack_recv.at[ry, rx],
            device_id={"depth": to}, device_id_type=MESH_ID)

    def add_in(first, num, place, terms):
        def one(i, c):
            total = mine[first + i, place]
            for term in terms:
                total = total + term(first + i)
            mine[first + i, place] = total
            return c
        lax.fori_loop(0, num, one, 0)

    for p in range(4):
        for g in turns:
            local_copy(p, g).start()
    pl.semaphore_wait(barrier, 18)
    for p in range(4):
        for g in turns:
            pair_copy(p, g).start()

    def take_pair(p, g):
        local_copy(p, g).wait()
        pair_copy(p, g).wait_recv()

    for g in turns:
        take_pair(0, g)
        add_in(row(g), 4, z_far, [lambda i: pair[i, z_far]])
        far_copy(g, 1).start()
        far_copy(g, 0).start()
    for g in turns:
        for p, to_up in ((1, 1), (2, 0)):
            take_pair(p, g)
            add_in(row(g), 4, places[p], [lambda i, p=p: pair[i, places[p]]])
            near_copy(g, to_up).start()
    for g in turns:
        for to_up in (1, 0):
            far_copy(g, to_up).wait_recv()
            via = via_up if to_up else via_down
            add_in(row(g) + 2 * (1 - to_up), 2, z_up if to_up else z_down, [lambda i, via=via: via[i]])
            sum_copy(g, to_up).start()
    for g in turns:
        take_pair(3, g)
        for to_up in (1, 0):
            near_copy(g, to_up).wait_recv()
            sum_copy(g, to_up).wait_recv()
        add_in(row(g), 4, z, [lambda i: pair[i, z], lambda i: from_up[i], lambda i: from_down[i]])
        for rx in (2, 1, 3, 0):
            if (g, rx) != (0, 0):
                stack_copy(g, rx).start()
    stack[d] = mine[d, z]
    for ry, rx in others:
        stack_copy(ry, rx).wait_recv()

    lane = lax.broadcasted_iota(jnp.int32, (32, 128), 1)

    def one_tile(t, c):
        def one_slab(p, carry):
            prior, light = carry
            value = stack[order_ref[p], t]
            own = jnp.where(lane >= 96, value, 0.0)
            twice = own + pltpu.roll(own, 32, 1)
            optical = twice + pltpu.roll(twice, 64, 1)
            light = light + jnp.exp(-(prior + 0.5 * optical)) * value
            return prior + optical, light
        zero = jnp.zeros((32, 128), jnp.float32)
        prior, light = lax.fori_loop(0, 16, one_slab, (zero, zero), unroll=4)
        image_ref[t] = jnp.where(lane >= 96, 1.0 - jnp.exp(-prior), light)
        return c
    lax.fori_loop(0, 4, one_tile, 0)

    for g in turns:
        for p in range(4):
            pair_copy(p, g).wait_send()
        for to_up in (1, 0):
            far_copy(g, to_up).wait_send()
            near_copy(g, to_up).wait_send()
            sum_copy(g, to_up).wait_send()
    for ry, rx in others:
        stack_copy(ry, rx).wait_send()


def exchange(partial_value, slab_rank):
    slots = jnp.arange(16, dtype=jnp.int32)
    order = jnp.sum(jnp.where(slab_rank[None, :] == slots[:, None], slots[None, :], 0), axis=1)
    dma = pltpu.SemaphoreType.DMA
    return pl.pallas_call(
        exchange_kernel,
        out_shape=jax.ShapeDtypeStruct((4, 32, 128), jnp.float32),
        in_specs=[pl.BlockSpec(memory_space=pltpu.SMEM), pl.BlockSpec(memory_space=pl.ANY)],
        out_specs=pl.BlockSpec(memory_space=pltpu.VMEM),
        scratch_shapes=[
            pltpu.VMEM((16, 4, 4, 32, 128), jnp.float32),
            pltpu.VMEM((16, 4, 4, 32, 128), jnp.float32),
            pltpu.VMEM((16, 4, 32, 128), jnp.float32),
            pltpu.VMEM((16, 4, 32, 128), jnp.float32),
            pltpu.VMEM((16, 4, 32, 128), jnp.float32),
            pltpu.VMEM((16, 4, 32, 128), jnp.float32),
            pltpu.VMEM((16, 4, 32, 128), jnp.float32),
            dma((4, 4)), dma((4, 4)), dma((4, 4)),
            dma((2, 4)), dma((2, 4)), dma((2, 4)), dma((2, 4)), dma((2, 4)), dma((2, 4)),
            dma((4, 4)), dma((4, 4)),
        ],
        compiler_params=pltpu.CompilerParams(collective_id=0, has_side_effects=True),
        name="exchange",
    )(order, partial_value.reshape(16, 4, 2, 4, 32, 128))


def shards(block_tile, block_count, slab_rank, corner, offset, radius, emission, extinction):
    partial_value = deposit_all(
        block_tile, block_count, corner, offset, radius, emission, extinction
    )
    return exchange(partial_value, slab_rank)


def solution(mesh):
    torus = Mesh(mesh.devices.reshape(mesh.shape["depth"], 4, 2), ("depth", "screen_0", "screen_1"))
    placed = (
        P("depth", SCREEN),
        P("depth", SCREEN),
        P(),
        P(None, "depth", SCREEN, None),
        P(None, "depth", SCREEN, None),
        P("depth", SCREEN, None),
        P(None, "depth", SCREEN, None),
        P("depth", SCREEN, None),
    )
    return jax.shard_map(
        shards, mesh=torus, in_specs=placed, out_specs=P(DEPTH_SCREEN, None, None), check_vma=False
    )
```

```python
import jax
import jax.numpy as jnp
from jax import lax
from jax.experimental import pallas as pl
from jax.experimental.pallas import tpu as pltpu
from jax.sharding import Mesh
from jax.sharding import PartitionSpec as P

SCREEN = ("screen_0", "screen_1")
DEPTH_SCREEN = ("depth", "screen_0", "screen_1")
BLK = 256
UNR = 64

def deposit_kernel(tile_ref, count_ref, corner_ref, offset_ref, radius_ref, emission_ref, extinction_ref, out_ref, pre_ref):
    step = pl.program_id(0)
    count = count_ref[0, 0]

    @pl.when(step == 0)
    def _():
        def zero(t, c):
            out_ref[t] = jnp.zeros(out_ref.shape[1:], jnp.float32)
            return c
        lax.fori_loop(0, out_ref.shape[0], zero, 0, unroll=8)

    first = step * BLK

    @pl.when(first < count)
    def _():
        slot = first + lax.broadcasted_iota(jnp.int32, (BLK, 128), 0)
        live = slot < count
        radius = radius_ref[0]
        h2 = radius * radius
        h4 = h2 * h2
        scale = jnp.where(live, 1.0 / (h4 * h4), 0.0)
        for k in range(2):
            edge = corner_ref[k, 0].astype(jnp.float32)
            pre_ref[2 * k] = edge
            pre_ref[2 * k + 1] = edge + 16.0 * offset_ref[k, 0] - 0.5
        pre_ref[4] = h2
        for c in range(3):
            pre_ref[5 + c] = emission_ref[c, 0] * scale
        pre_ref[8] = extinction_ref[0] * scale

        rows = lax.broadcasted_iota(jnp.int32, (16, 128), 0).astype(jnp.float32)
        rows16 = rows.astype(jnp.bfloat16)
        zero16 = jnp.zeros((16, 128), jnp.bfloat16)

        def split(w):
            high = w.astype(jnp.bfloat16)
            low = (w - high.astype(jnp.float32)).astype(jnp.bfloat16)
            return high, low

        def one_group(g, c):
            outs = []
            for u in range(UNR):
                j = g * UNR + u
                def row(a):
                    return jnp.broadcast_to(pre_ref[a, pl.ds(j, 1), :], (16, 128))
                h2r = row(4)
                def bump(k):
                    edge = row(2 * k)
                    mask16 = rows16 < edge.astype(jnp.bfloat16)
                    at = jnp.where(rows < edge, rows + 16.0, rows)
                    s = at - row(2 * k + 1)
                    v = jnp.maximum(h2r - s * s, 0.0)
                    return v * v, mask16
                wx, mx = bump(0)
                wy, my = bump(1)
                def spread(w16, m):
                    return [jnp.where(m, zero16, w16), jnp.where(m, w16, zero16)]
                yh, yl = split(wy)
                lhs = jnp.concatenate(spread(yh, my) + spread(yl, my), 0)
                lhs = jnp.concatenate([lhs, lhs], 1)
                hi, lo = [], []
                for ch in range(4):
                    a, b = split(row(5 + ch) * wx)
                    hi += spread(a, mx)
                    lo += spread(b, mx)
                rhs = jnp.concatenate([jnp.concatenate(hi, 0), jnp.concatenate(lo, 0)], 1)
                outs.append(lax.dot_general(lhs, rhs, (((1,), (1,)), ((), ())), preferred_element_type=jnp.float32))
            for u in range(UNR):
                t = tile_ref[0, first + g * UNR + u]
                out_ref[t] += outs[u][:32] + outs[u][32:]
            return c

        groups = lax.div(jnp.minimum(count - first, BLK) + (UNR - 1), UNR)
        lax.fori_loop(0, groups, one_group, 0)


def deposit_all(block_tile, block_count, corner, offset, radius, emission, extinction, tiles=512):
    slots = block_tile.shape[1]
    steps = slots // BLK
    def last(i, tile, count):
        return jnp.minimum(i, lax.div(count[0, 0] - 1, BLK))
    def m4(n):
        return pl.BlockSpec((n, 1, BLK, 128), lambda i, t, c: (0, 0, last(i, t, c), 0))
    def m3():
        return pl.BlockSpec((1, BLK, 128), lambda i, t, c: (0, last(i, t, c), 0))
    return pl.pallas_call(
        deposit_kernel,
        out_shape=jax.ShapeDtypeStruct((tiles, 32, 128), jnp.float32),
        grid_spec=pltpu.PrefetchScalarGridSpec(
            num_scalar_prefetch=2, grid=(steps,),
            in_specs=[m4(2), m4(2), m3(), m4(3), m3()],
            out_specs=pl.BlockSpec((tiles, 32, 128), lambda i, t, c: (0, 0, 0)),
            scratch_shapes=[pltpu.VMEM((9, BLK, 128), jnp.float32)],
        ),
        compiler_params=pltpu.CompilerParams(dimension_semantics=("arbitrary",)),
        name="deposit",
    )(block_tile, block_count, corner, offset, radius, emission, extinction)


MESH_ID = pl.DeviceIdType.MESH


def exchange_kernel(rank_ref, partial_ref, image_ref, order_ref, mine, pair, from_up, from_down, via_up, via_down, stack,
                    local_sem, pair_send, pair_recv, far_send, far_recv, near_send, near_recv, sum_send, sum_recv,
                    stack_send, stack_recv):
    d = lax.axis_index("depth")
    z = lax.axis_index("screen_0")
    core = lax.axis_index("screen_1")
    mate = 1 - core
    y, x = lax.div(d, 4), lax.rem(d, 4)
    z_up, z_down, z_far = lax.rem(z + 1, 4), lax.rem(z + 3, 4), lax.rem(z + 2, 4)
    turns = (2, 1, 3, 0)
    others = [(ry, rx) for ry in turns for rx in (2, 1, 3, 0) if (ry, rx) != (0, 0)]

    def away(ry, rx):
        return lax.rem(y + ry, 4) * 4 + lax.rem(x + rx, 4)

    def row(ry):
        return lax.rem(y + ry, 4) * 4

    barrier = pltpu.get_barrier_semaphore()
    pl.semaphore_signal(barrier, inc=1, device_id={"screen_1": mate}, device_id_type=MESH_ID)
    pl.semaphore_signal(barrier, inc=1, device_id={"screen_0": z_up}, device_id_type=MESH_ID)
    pl.semaphore_signal(barrier, inc=1, device_id={"screen_0": z_down}, device_id_type=MESH_ID)
    for ry, rx in others:
        pl.semaphore_signal(barrier, inc=1, device_id={"depth": away(ry, rx)}, device_id_type=MESH_ID)

    places = (z_far, z_up, z_down, z)

    def local_copy(p, g):
        rows = pl.ds(row(g), 4)
        return pltpu.make_async_copy(
            partial_ref.at[rows, places[p], core], mine.at[rows, places[p]], local_sem.at[p, g])

    def pair_copy(p, g):
        rows = pl.ds(row(g), 4)
        return pltpu.make_async_remote_copy(
            partial_ref.at[rows, places[p], mate], pair.at[rows, places[p]],
            pair_send.at[p, g], pair_recv.at[p, g], device_id={"screen_1": mate}, device_id_type=MESH_ID)

    def line_copy(g, half, place, goal, to_up, send, recv):
        rows = pl.ds(row(g) + 2 * half, 2)
        return pltpu.make_async_remote_copy(
            mine.at[rows, place], goal.at[rows], send.at[to_up, g], recv.at[to_up, g],
            device_id={"screen_0": z_up if to_up else z_down}, device_id_type=MESH_ID)

    def far_copy(g, to_up):
        return line_copy(g, 1 - to_up, z_far, via_up if to_up else via_down, to_up, far_send, far_recv)

    def near_copy(g, to_up):
        return line_copy(g, to_up, z_up if to_up else z_down, from_up if to_up else from_down, to_up,
                         near_send, near_recv)

    def sum_copy(g, to_up):
        return line_copy(g, 1 - to_up, z_up if to_up else z_down, from_up if to_up else from_down, to_up,
                         sum_send, sum_recv)

    def stack_copy(ry, rx):
        to = away(ry, rx)
        return pltpu.make_async_remote_copy(
            mine.at[to, z], stack.at[d], stack_send.at[ry, rx], stack_recv.at[ry, rx],
            device_id={"depth": to}, device_id_type=MESH_ID)

    def add_in(first, num, place, terms):
        def one(i, c):
            total = mine[first + i, place]
            for term in terms:
                total = total + term(first + i)
            mine[first + i, place] = total
            return c
        lax.fori_loop(0, num, one, 0)

    for p in range(4):
        for g in turns:
            local_copy(p, g).start()
    pl.semaphore_wait(barrier, 18)
    for p in range(4):
        for g in turns:
            pair_copy(p, g).start()

    for p in range(16):
        slab = 0
        for j in range(1, 16):
            slab = jnp.where(rank_ref[j] == p, j, slab)
        order_ref[p] = slab

    def take_pair(p, g):
        local_copy(p, g).wait()
        pair_copy(p, g).wait_recv()

    for g in turns:
        take_pair(0, g)
        add_in(row(g), 4, z_far, [lambda i: pair[i, z_far]])
        far_copy(g, 1).start()
        far_copy(g, 0).start()
    for g in turns:
        for p, to_up in ((1, 1), (2, 0)):
            take_pair(p, g)
            add_in(row(g), 4, places[p], [lambda i, p=p: pair[i, places[p]]])
            near_copy(g, to_up).start()
    for g in turns:
        for to_up in (1, 0):
            far_copy(g, to_up).wait_recv()
            via = via_up if to_up else via_down
            add_in(row(g) + 2 * (1 - to_up), 2, z_up if to_up else z_down, [lambda i, via=via: via[i]])
            sum_copy(g, to_up).start()
    for g in turns:
        take_pair(3, g)
        for to_up in (1, 0):
            near_copy(g, to_up).wait_recv()
            sum_copy(g, to_up).wait_recv()
        add_in(row(g), 4, z, [lambda i: pair[i, z], lambda i: from_up[i], lambda i: from_down[i]])
        for rx in (2, 1, 3, 0):
            if (g, rx) != (0, 0):
                stack_copy(g, rx).start()
    stack[d] = mine[d, z]
    for ry, rx in others:
        stack_copy(ry, rx).wait_recv()

    lane = lax.broadcasted_iota(jnp.int32, (32, 128), 1)

    def one_tile(t, c):
        def one_slab(p, carry):
            prior, light = carry
            value = stack[order_ref[p], t]
            own = jnp.where(lane >= 96, value, 0.0)
            twice = own + pltpu.roll(own, 32, 1)
            optical = twice + pltpu.roll(twice, 64, 1)
            light = light + jnp.exp(-(prior + 0.5 * optical)) * value
            return prior + optical, light
        zero = jnp.zeros((32, 128), jnp.float32)
        prior, light = lax.fori_loop(0, 16, one_slab, (zero, zero), unroll=4)
        image_ref[t] = jnp.where(lane >= 96, 1.0 - jnp.exp(-prior), light)
        return c
    lax.fori_loop(0, 4, one_tile, 0)

    for g in turns:
        for p in range(4):
            pair_copy(p, g).wait_send()
        for to_up in (1, 0):
            far_copy(g, to_up).wait_send()
            near_copy(g, to_up).wait_send()
            sum_copy(g, to_up).wait_send()
    for ry, rx in others:
        stack_copy(ry, rx).wait_send()


def exchange(partial_value, slab_rank):
    dma = pltpu.SemaphoreType.DMA
    return pl.pallas_call(
        exchange_kernel,
        out_shape=jax.ShapeDtypeStruct((4, 32, 128), jnp.float32),
        in_specs=[pl.BlockSpec(memory_space=pltpu.SMEM), pl.BlockSpec(memory_space=pl.ANY)],
        out_specs=pl.BlockSpec(memory_space=pltpu.VMEM),
        scratch_shapes=[
            pltpu.SMEM((16,), jnp.int32),
            pltpu.VMEM((16, 4, 4, 32, 128), jnp.float32),
            pltpu.VMEM((16, 4, 4, 32, 128), jnp.float32),
            pltpu.VMEM((16, 4, 32, 128), jnp.float32),
            pltpu.VMEM((16, 4, 32, 128), jnp.float32),
            pltpu.VMEM((16, 4, 32, 128), jnp.float32),
            pltpu.VMEM((16, 4, 32, 128), jnp.float32),
            pltpu.VMEM((16, 4, 32, 128), jnp.float32),
            dma((4, 4)), dma((4, 4)), dma((4, 4)),
            dma((2, 4)), dma((2, 4)), dma((2, 4)), dma((2, 4)), dma((2, 4)), dma((2, 4)),
            dma((4, 4)), dma((4, 4)),
        ],
        compiler_params=pltpu.CompilerParams(collective_id=0, has_side_effects=True),
        name="exchange",
    )(slab_rank, partial_value.reshape(16, 4, 2, 4, 32, 128))


def shards(block_tile, block_count, slab_rank, corner, offset, radius, emission, extinction):
    partial_value = deposit_all(
        block_tile, block_count, corner, offset, radius, emission, extinction
    )
    return exchange(partial_value, slab_rank)


def solution(mesh):
    torus = Mesh(mesh.devices.reshape(mesh.shape["depth"], 4, 2), ("depth", "screen_0", "screen_1"))
    placed = (
        P("depth", SCREEN),
        P("depth", SCREEN),
        P(),
        P(None, "depth", SCREEN, None),
        P(None, "depth", SCREEN, None),
        P("depth", SCREEN, None),
        P(None, "depth", SCREEN, None),
        P("depth", SCREEN, None),
    )
    return jax.shard_map(
        shards, mesh=torus, in_specs=placed, out_specs=P(DEPTH_SCREEN, None, None), check_vma=False
    )
```

```python
import functools

import jax
import jax.numpy as jnp
from jax import lax
from jax.experimental import pallas as pl
from jax.experimental.pallas import tpu as pltpu
from jax.sharding import Mesh
from jax.sharding import PartitionSpec as P

SCREEN = ("screen_0", "screen_1")
DEPTH_SCREEN = ("depth", "screen_0", "screen_1")
BLK = 256
UNR = 64

KEPT = 1536
MESH_ID = pl.DeviceIdType.MESH


def share_kernel(tile_ref, count_ref, corner_ref, offset_ref, radius_ref, emission_ref, extinction_ref,
                 tile_out, count_out, corner_out, offset_out, radius_out, emission_out, extinction_out,
                 send_sem, recv_sem):
    mate = 1 - lax.axis_index("screen_1")
    barrier = pltpu.get_barrier_semaphore()
    pl.semaphore_signal(barrier, inc=1, device_id={"screen_1": mate}, device_id_type=MESH_ID)
    pl.semaphore_wait(barrier, 1)
    given = pl.ds(KEPT, tile_ref.shape[1] - KEPT)
    pairs = [
        (tile_ref.at[:, given], tile_out),
        (count_ref, count_out),
        (corner_ref.at[0, :, given], corner_out.at[0]),
        (corner_ref.at[1, :, given], corner_out.at[1]),
        (offset_ref.at[0, :, given], offset_out.at[0]),
        (offset_ref.at[1, :, given], offset_out.at[1]),
        (radius_ref.at[:, given], radius_out),
        (emission_ref.at[0, :, given], emission_out.at[0]),
        (emission_ref.at[1, :, given], emission_out.at[1]),
        (emission_ref.at[2, :, given], emission_out.at[2]),
        (extinction_ref.at[:, given], extinction_out),
    ]
    copies = [
        pltpu.make_async_remote_copy(
            source, goal, send_sem.at[n], recv_sem.at[n], device_id={"screen_1": mate}, device_id_type=MESH_ID)
        for n, (source, goal) in enumerate(pairs)
    ]
    for copy in copies:
        copy.start()
    for copy in copies:
        copy.wait()


def share(block_tile, block_count, corner, offset, radius, emission, extinction):
    num = block_tile.shape[1] - KEPT
    any_spec = pl.BlockSpec(memory_space=pl.ANY)
    def cut(n, dtype):
        return jax.ShapeDtypeStruct((n, 1, num, 128), dtype)
    flat = jax.ShapeDtypeStruct((1, num, 128), jnp.float32)
    return pl.pallas_call(
        share_kernel,
        out_shape=[
            jax.ShapeDtypeStruct((1, num), jnp.int32),
            jax.ShapeDtypeStruct(block_count.shape, jnp.int32),
            cut(2, jnp.int32), cut(2, jnp.float32), flat, cut(3, jnp.float32), flat,
        ],
        in_specs=[any_spec] * 7,
        out_specs=[any_spec] * 7,
        scratch_shapes=[pltpu.SemaphoreType.DMA((11,)), pltpu.SemaphoreType.DMA((11,))],
        compiler_params=pltpu.CompilerParams(collective_id=1, has_side_effects=True),
        name="share",
    )(block_tile, block_count, corner, offset, radius, emission, extinction)


def deposit_kernel(own_steps, tile_ref, count_ref, mate_tile_ref, mate_count_ref, *refs):
    own_refs, mate_refs, (out_ref, pre_ref) = refs[:5], refs[5:10], refs[10:]
    step = pl.program_id(0)
    own = step < own_steps
    first = jnp.minimum(step, own_steps - 1) * BLK
    mate_first = jnp.maximum(step - own_steps, 0) * BLK
    own_live = jnp.minimum(count_ref[0, 0], own_steps * BLK) - first
    mate_live = mate_count_ref[0, 0] - own_steps * BLK - mate_first
    live_num = jnp.where(own, own_live, mate_live)

    @pl.when(step == 0)
    def _():
        def zero(t, c):
            out_ref[t] = jnp.zeros(out_ref.shape[1:], jnp.float32)
            return c
        lax.fori_loop(0, out_ref.shape[0], zero, 0, unroll=8)

    def prepare(corner_ref, offset_ref, radius_ref, emission_ref, extinction_ref):
        live = lax.broadcasted_iota(jnp.int32, (BLK, 128), 0) < live_num
        radius = radius_ref[0]
        h2 = radius * radius
        h4 = h2 * h2
        scale = jnp.where(live, 1.0 / (h4 * h4), 0.0)
        for k in range(2):
            edge = corner_ref[k, 0].astype(jnp.float32)
            pre_ref[2 * k] = edge
            pre_ref[2 * k + 1] = edge + 16.0 * offset_ref[k, 0] - 0.5
        pre_ref[4] = h2
        for c in range(3):
            pre_ref[5 + c] = emission_ref[c, 0] * scale
        pre_ref[8] = extinction_ref[0] * scale

    @pl.when(jnp.logical_and(own, live_num > 0))
    def _():
        prepare(*own_refs)

    @pl.when(jnp.logical_and(jnp.logical_not(own), live_num > 0))
    def _():
        prepare(*mate_refs)

    @pl.when(live_num > 0)
    def _():
        rows = lax.broadcasted_iota(jnp.int32, (16, 128), 0).astype(jnp.float32)
        rows16 = rows.astype(jnp.bfloat16)
        zero16 = jnp.zeros((16, 128), jnp.bfloat16)

        def split(w):
            high = w.astype(jnp.bfloat16)
            low = (w - high.astype(jnp.float32)).astype(jnp.bfloat16)
            return high, low

        def one_group(g, c):
            outs = []
            for u in range(UNR):
                j = g * UNR + u
                def row(a):
                    return jnp.broadcast_to(pre_ref[a, pl.ds(j, 1), :], (16, 128))
                h2r = row(4)
                def bump(k):
                    edge = row(2 * k)
                    mask16 = rows16 < edge.astype(jnp.bfloat16)
                    at = jnp.where(rows < edge, rows + 16.0, rows)
                    s = at - row(2 * k + 1)
                    v = jnp.maximum(h2r - s * s, 0.0)
                    return v * v, mask16
                wx, mx = bump(0)
                wy, my = bump(1)
                def spread(w16, m):
                    return [jnp.where(m, zero16, w16), jnp.where(m, w16, zero16)]
                yh, yl = split(wy)
                lhs = jnp.concatenate(spread(yh, my) + spread(yl, my), 0)
                lhs = jnp.concatenate([lhs, lhs], 1)
                hi, lo = [], []
                for ch in range(4):
                    a, b = split(row(5 + ch) * wx)
                    hi += spread(a, mx)
                    lo += spread(b, mx)
                rhs = jnp.concatenate([jnp.concatenate(hi, 0), jnp.concatenate(lo, 0)], 1)
                outs.append(lax.dot_general(lhs, rhs, (((1,), (1,)), ((), ())), preferred_element_type=jnp.float32))
            for u in range(UNR):
                t = jnp.where(own, tile_ref[0, first + g * UNR + u], mate_tile_ref[0, mate_first + g * UNR + u])
                out_ref[t] += outs[u][:32] + outs[u][32:]
            return c

        groups = lax.div(jnp.minimum(live_num, BLK) + (UNR - 1), UNR)
        lax.fori_loop(0, groups, one_group, 0)


def deposit_all(block_tile, block_count, corner, offset, radius, emission, extinction, tiles=512):
    mate_tile, mate_count, *mate_rest = share(block_tile, block_count, corner, offset, radius, emission, extinction)
    own_steps = KEPT // BLK
    steps = block_tile.shape[1] // BLK
    def own_at(i, tile, count, *unused):
        return jnp.minimum(jnp.minimum(i, own_steps - 1), lax.div(count[0, 0] - 1, BLK))
    def mate_at(i, *unused):
        return jnp.maximum(i - own_steps, 0)
    def specs(at):
        def m4(n):
            return pl.BlockSpec((n, 1, BLK, 128), lambda i, *scalars: (0, 0, at(i, *scalars), 0))
        def m3():
            return pl.BlockSpec((1, BLK, 128), lambda i, *scalars: (0, at(i, *scalars), 0))
        return [m4(2), m4(2), m3(), m4(3), m3()]
    return pl.pallas_call(
        functools.partial(deposit_kernel, own_steps),
        out_shape=jax.ShapeDtypeStruct((tiles, 32, 128), jnp.float32),
        grid_spec=pltpu.PrefetchScalarGridSpec(
            num_scalar_prefetch=4, grid=(steps,),
            in_specs=specs(own_at) + specs(mate_at),
            out_specs=pl.BlockSpec((tiles, 32, 128), lambda i, *scalars: (0, 0, 0)),
            scratch_shapes=[pltpu.VMEM((9, BLK, 128), jnp.float32)],
        ),
        compiler_params=pltpu.CompilerParams(dimension_semantics=("arbitrary",)),
        name="deposit",
    )(block_tile, block_count, mate_tile, mate_count, corner, offset, radius, emission, extinction, *mate_rest)


def exchange_kernel(rank_ref, partial_ref, image_ref, order_ref, mine, pair, from_up, from_down, via_up, via_down, stack,
                    local_sem, pair_send, pair_recv, far_send, far_recv, near_send, near_recv, sum_send, sum_recv,
                    stack_send, stack_recv):
    d = lax.axis_index("depth")
    z = lax.axis_index("screen_0")
    core = lax.axis_index("screen_1")
    mate = 1 - core
    y, x = lax.div(d, 4), lax.rem(d, 4)
    z_up, z_down, z_far = lax.rem(z + 1, 4), lax.rem(z + 3, 4), lax.rem(z + 2, 4)
    turns = (2, 1, 3, 0)
    others = [(ry, rx) for ry in turns for rx in (2, 1, 3, 0) if (ry, rx) != (0, 0)]

    def away(ry, rx):
        return lax.rem(y + ry, 4) * 4 + lax.rem(x + rx, 4)

    def row(ry):
        return lax.rem(y + ry, 4) * 4

    barrier = pltpu.get_barrier_semaphore()
    pl.semaphore_signal(barrier, inc=1, device_id={"screen_1": mate}, device_id_type=MESH_ID)
    pl.semaphore_signal(barrier, inc=1, device_id={"screen_0": z_up}, device_id_type=MESH_ID)
    pl.semaphore_signal(barrier, inc=1, device_id={"screen_0": z_down}, device_id_type=MESH_ID)
    for ry, rx in others:
        pl.semaphore_signal(barrier, inc=1, device_id={"depth": away(ry, rx)}, device_id_type=MESH_ID)

    places = (z_far, z_up, z_down, z)

    def local_copy(p, g):
        rows = pl.ds(row(g), 4)
        return pltpu.make_async_copy(
            partial_ref.at[rows, places[p], core], mine.at[rows, places[p]], local_sem.at[p, g])

    def pair_copy(p, g):
        rows = pl.ds(row(g), 4)
        return pltpu.make_async_remote_copy(
            partial_ref.at[rows, places[p], mate], pair.at[rows, places[p]],
            pair_send.at[p, g], pair_recv.at[p, g], device_id={"screen_1": mate}, device_id_type=MESH_ID)

    def line_copy(g, half, place, goal, to_up, send, recv):
        rows = pl.ds(row(g) + 2 * half, 2)
        return pltpu.make_async_remote_copy(
            mine.at[rows, place], goal.at[rows], send.at[to_up, g], recv.at[to_up, g],
            device_id={"screen_0": z_up if to_up else z_down}, device_id_type=MESH_ID)

    def far_copy(g, to_up):
        return line_copy(g, 1 - to_up, z_far, via_up if to_up else via_down, to_up, far_send, far_recv)

    def near_copy(g, to_up):
        return line_copy(g, to_up, z_up if to_up else z_down, from_up if to_up else from_down, to_up,
                         near_send, near_recv)

    def sum_copy(g, to_up):
        return line_copy(g, 1 - to_up, z_up if to_up else z_down, from_up if to_up else from_down, to_up,
                         sum_send, sum_recv)

    def stack_copy(ry, rx):
        to = away(ry, rx)
        return pltpu.make_async_remote_copy(
            mine.at[to, z], stack.at[d], stack_send.at[ry, rx], stack_recv.at[ry, rx],
            device_id={"depth": to}, device_id_type=MESH_ID)

    def add_in(first, num, place, terms):
        def one(i, c):
            total = mine[first + i, place]
            for term in terms:
                total = total + term(first + i)
            mine[first + i, place] = total
            return c
        lax.fori_loop(0, num, one, 0)

    for p in range(4):
        for g in turns:
            local_copy(p, g).start()
    pl.semaphore_wait(barrier, 18)
    for p in range(4):
        for g in turns:
            pair_copy(p, g).start()

    for p in range(16):
        slab = 0
        for j in range(1, 16):
            slab = jnp.where(rank_ref[j] == p, j, slab)
        order_ref[p] = slab

    def take_pair(p, g):
        local_copy(p, g).wait()
        pair_copy(p, g).wait_recv()

    for g in turns:
        take_pair(0, g)
        add_in(row(g), 4, z_far, [lambda i: pair[i, z_far]])
        far_copy(g, 1).start()
        far_copy(g, 0).start()
    for g in turns:
        for p, to_up in ((1, 1), (2, 0)):
            take_pair(p, g)
            add_in(row(g), 4, places[p], [lambda i, p=p: pair[i, places[p]]])
            near_copy(g, to_up).start()
    for g in turns:
        for to_up in (1, 0):
            far_copy(g, to_up).wait_recv()
            via = via_up if to_up else via_down
            add_in(row(g) + 2 * (1 - to_up), 2, z_up if to_up else z_down, [lambda i, via=via: via[i]])
            sum_copy(g, to_up).start()
    for g in turns:
        take_pair(3, g)
        for to_up in (1, 0):
            near_copy(g, to_up).wait_recv()
            sum_copy(g, to_up).wait_recv()
        add_in(row(g), 4, z, [lambda i: pair[i, z], lambda i: from_up[i], lambda i: from_down[i]])
        for rx in (2, 1, 3, 0):
            if (g, rx) != (0, 0):
                stack_copy(g, rx).start()
    stack[d] = mine[d, z]
    for ry, rx in others:
        stack_copy(ry, rx).wait_recv()

    lane = lax.broadcasted_iota(jnp.int32, (32, 128), 1)

    def one_tile(t, c):
        def one_slab(p, carry):
            prior, light = carry
            value = stack[order_ref[p], t]
            own = jnp.where(lane >= 96, value, 0.0)
            twice = own + pltpu.roll(own, 32, 1)
            optical = twice + pltpu.roll(twice, 64, 1)
            light = light + jnp.exp(-(prior + 0.5 * optical)) * value
            return prior + optical, light
        zero = jnp.zeros((32, 128), jnp.float32)
        prior, light = lax.fori_loop(0, 16, one_slab, (zero, zero), unroll=4)
        image_ref[t] = jnp.where(lane >= 96, 1.0 - jnp.exp(-prior), light)
        return c
    lax.fori_loop(0, 4, one_tile, 0)

    for g in turns:
        for p in range(4):
            pair_copy(p, g).wait_send()
        for to_up in (1, 0):
            far_copy(g, to_up).wait_send()
            near_copy(g, to_up).wait_send()
            sum_copy(g, to_up).wait_send()
    for ry, rx in others:
        stack_copy(ry, rx).wait_send()


def exchange(partial_value, slab_rank):
    dma = pltpu.SemaphoreType.DMA
    return pl.pallas_call(
        exchange_kernel,
        out_shape=jax.ShapeDtypeStruct((4, 32, 128), jnp.float32),
        in_specs=[pl.BlockSpec(memory_space=pltpu.SMEM), pl.BlockSpec(memory_space=pl.ANY)],
        out_specs=pl.BlockSpec(memory_space=pltpu.VMEM),
        scratch_shapes=[
            pltpu.SMEM((16,), jnp.int32),
            pltpu.VMEM((16, 4, 4, 32, 128), jnp.float32),
            pltpu.VMEM((16, 4, 4, 32, 128), jnp.float32),
            pltpu.VMEM((16, 4, 32, 128), jnp.float32),
            pltpu.VMEM((16, 4, 32, 128), jnp.float32),
            pltpu.VMEM((16, 4, 32, 128), jnp.float32),
            pltpu.VMEM((16, 4, 32, 128), jnp.float32),
            pltpu.VMEM((16, 4, 32, 128), jnp.float32),
            dma((4, 4)), dma((4, 4)), dma((4, 4)),
            dma((2, 4)), dma((2, 4)), dma((2, 4)), dma((2, 4)), dma((2, 4)), dma((2, 4)),
            dma((4, 4)), dma((4, 4)),
        ],
        compiler_params=pltpu.CompilerParams(collective_id=0, has_side_effects=True),
        name="exchange",
    )(slab_rank, partial_value.reshape(16, 4, 2, 4, 32, 128))


def shards(block_tile, block_count, slab_rank, corner, offset, radius, emission, extinction):
    partial_value = deposit_all(
        block_tile, block_count, corner, offset, radius, emission, extinction
    )
    return exchange(partial_value, slab_rank)


def solution(mesh):
    torus = Mesh(mesh.devices.reshape(mesh.shape["depth"], 4, 2), ("depth", "screen_0", "screen_1"))
    placed = (
        P("depth", SCREEN),
        P("depth", SCREEN),
        P(),
        P(None, "depth", SCREEN, None),
        P(None, "depth", SCREEN, None),
        P("depth", SCREEN, None),
        P(None, "depth", SCREEN, None),
        P("depth", SCREEN, None),
    )
    return jax.shard_map(
        shards, mesh=torus, in_specs=placed, out_specs=P(DEPTH_SCREEN, None, None), check_vma=False
    )
```

```python
import functools

import jax
import jax.numpy as jnp
from jax import lax
from jax.experimental import pallas as pl
from jax.experimental.pallas import tpu as pltpu
from jax.sharding import Mesh
from jax.sharding import PartitionSpec as P

SCREEN = ("screen_0", "screen_1")
DEPTH_SCREEN = ("depth", "screen_0", "screen_1")
BLK = 256
UNR = 64

KEPT = 1536
MESH_ID = pl.DeviceIdType.MESH


def share_kernel(tile_ref, count_ref, corner_ref, offset_ref, radius_ref, emission_ref, extinction_ref,
                 tile_out, count_out, corner_out, offset_out, radius_out, emission_out, extinction_out,
                 send_sem, recv_sem):
    mate = 1 - lax.axis_index("screen_1")
    barrier = pltpu.get_barrier_semaphore()
    pl.semaphore_signal(barrier, inc=1, device_id={"screen_1": mate}, device_id_type=MESH_ID)
    pl.semaphore_wait(barrier, 1)
    given = pl.ds(KEPT, tile_ref.shape[1] - KEPT)
    pairs = [
        (tile_ref.at[:, given], tile_out),
        (count_ref, count_out),
        (corner_ref.at[0, :, given], corner_out.at[0]),
        (corner_ref.at[1, :, given], corner_out.at[1]),
        (offset_ref.at[0, :, given], offset_out.at[0]),
        (offset_ref.at[1, :, given], offset_out.at[1]),
        (radius_ref.at[:, given], radius_out),
        (emission_ref.at[0, :, given], emission_out.at[0]),
        (emission_ref.at[1, :, given], emission_out.at[1]),
        (emission_ref.at[2, :, given], emission_out.at[2]),
        (extinction_ref.at[:, given], extinction_out),
    ]
    copies = [
        pltpu.make_async_remote_copy(
            source, goal, send_sem.at[n], recv_sem.at[n], device_id={"screen_1": mate}, device_id_type=MESH_ID)
        for n, (source, goal) in enumerate(pairs)
    ]
    for copy in copies:
        copy.start()
    for copy in copies:
        copy.wait()


def share(block_tile, block_count, corner, offset, radius, emission, extinction):
    num = block_tile.shape[1] - KEPT
    any_spec = pl.BlockSpec(memory_space=pl.ANY)
    def cut(n, dtype):
        return jax.ShapeDtypeStruct((n, 1, num, 128), dtype)
    flat = jax.ShapeDtypeStruct((1, num, 128), jnp.float32)
    return pl.pallas_call(
        share_kernel,
        out_shape=[
            jax.ShapeDtypeStruct((1, num), jnp.int32),
            jax.ShapeDtypeStruct(block_count.shape, jnp.int32),
            cut(2, jnp.int32), cut(2, jnp.float32), flat, cut(3, jnp.float32), flat,
        ],
        in_specs=[any_spec] * 7,
        out_specs=[any_spec] * 7,
        scratch_shapes=[pltpu.SemaphoreType.DMA((11,)), pltpu.SemaphoreType.DMA((11,))],
        compiler_params=pltpu.CompilerParams(collective_id=1, has_side_effects=True),
        name="share",
    )(block_tile, block_count, corner, offset, radius, emission, extinction)


def deposit_kernel(own_steps, tile_ref, count_ref, mate_tile_ref, mate_count_ref, *refs):
    own_refs, mate_refs, (out_ref, pre_ref) = refs[:5], refs[5:10], refs[10:]
    step = pl.program_id(0)
    own = step < own_steps
    first = jnp.minimum(step, own_steps - 1) * BLK
    mate_first = jnp.maximum(step - own_steps, 0) * BLK
    own_live = jnp.minimum(count_ref[0, 0], own_steps * BLK) - first
    mate_live = mate_count_ref[0, 0] - own_steps * BLK - mate_first
    live_num = jnp.where(own, own_live, mate_live)

    @pl.when(step == 0)
    def _():
        def zero(t, c):
            out_ref[t] = jnp.zeros(out_ref.shape[1:], jnp.float32)
            return c
        lax.fori_loop(0, out_ref.shape[0], zero, 0, unroll=8)

    def prepare(corner_ref, offset_ref, radius_ref, emission_ref, extinction_ref):
        live = lax.broadcasted_iota(jnp.int32, (BLK, 128), 0) < live_num
        radius = radius_ref[0]
        h2 = radius * radius
        h4 = h2 * h2
        scale = jnp.where(live, 1.0 / (h4 * h4), 0.0)
        for k in range(2):
            edge = corner_ref[k, 0].astype(jnp.float32)
            pre_ref[2 * k] = edge
            pre_ref[2 * k + 1] = edge + 16.0 * offset_ref[k, 0] - 0.5
        pre_ref[4] = h2
        for c in range(3):
            pre_ref[5 + c] = emission_ref[c, 0] * scale
        pre_ref[8] = extinction_ref[0] * scale

    @pl.when(jnp.logical_and(own, live_num > 0))
    def _():
        prepare(*own_refs)

    @pl.when(jnp.logical_and(jnp.logical_not(own), live_num > 0))
    def _():
        prepare(*mate_refs)

    @pl.when(live_num > 0)
    def _():
        rows = lax.broadcasted_iota(jnp.int32, (16, 128), 0).astype(jnp.float32)
        rows16 = rows.astype(jnp.bfloat16)
        zero16 = jnp.zeros((16, 128), jnp.bfloat16)

        def split(w):
            high = w.astype(jnp.bfloat16)
            low = (w - high.astype(jnp.float32)).astype(jnp.bfloat16)
            return high, low

        def one_group(g, c):
            outs = []
            for u in range(UNR):
                j = g * UNR + u
                def row(a):
                    return jnp.broadcast_to(pre_ref[a, pl.ds(j, 1), :], (16, 128))
                h2r = row(4)
                def bump(k):
                    edge = row(2 * k)
                    mask16 = rows16 < edge.astype(jnp.bfloat16)
                    at = jnp.where(rows < edge, rows + 16.0, rows)
                    s = at - row(2 * k + 1)
                    v = jnp.maximum(h2r - s * s, 0.0)
                    return v * v, mask16
                wx, mx = bump(0)
                wy, my = bump(1)
                def spread(w16, m):
                    return [jnp.where(m, zero16, w16), jnp.where(m, w16, zero16)]
                yh, yl = split(wy)
                lhs = jnp.concatenate(spread(yh, my) + spread(yl, my), 0)
                lhs = jnp.concatenate([lhs, lhs], 1)
                hi, lo = [], []
                for ch in range(4):
                    a, b = split(row(5 + ch) * wx)
                    hi += spread(a, mx)
                    lo += spread(b, mx)
                rhs = jnp.concatenate([jnp.concatenate(hi, 0), jnp.concatenate(lo, 0)], 1)
                outs.append(lax.dot_general(lhs, rhs, (((1,), (1,)), ((), ())), preferred_element_type=jnp.float32))
            for u in range(UNR):
                t = jnp.where(own, tile_ref[0, first + g * UNR + u], mate_tile_ref[0, mate_first + g * UNR + u])
                out_ref[t] += outs[u][:32] + outs[u][32:]
            return c

        groups = lax.div(jnp.minimum(live_num, BLK) + (UNR - 1), UNR)
        lax.fori_loop(0, groups, one_group, 0)


def deposit_all(block_tile, block_count, corner, offset, radius, emission, extinction, tiles=512):
    mate_tile, mate_count, *mate_rest = share(block_tile, block_count, corner, offset, radius, emission, extinction)
    own_steps = KEPT // BLK
    steps = block_tile.shape[1] // BLK
    def own_at(i, tile, count, *unused):
        return jnp.minimum(jnp.minimum(i, own_steps - 1), lax.div(count[0, 0] - 1, BLK))
    def mate_at(i, *unused):
        return jnp.maximum(i - own_steps, 0)
    def specs(at):
        def m4(n):
            return pl.BlockSpec((n, 1, BLK, 128), lambda i, *scalars: (0, 0, at(i, *scalars), 0))
        def m3():
            return pl.BlockSpec((1, BLK, 128), lambda i, *scalars: (0, at(i, *scalars), 0))
        return [m4(2), m4(2), m3(), m4(3), m3()]
    return pl.pallas_call(
        functools.partial(deposit_kernel, own_steps),
        out_shape=pltpu.VMEM((tiles, 32, 128), jnp.float32),
        grid_spec=pltpu.PrefetchScalarGridSpec(
            num_scalar_prefetch=4, grid=(steps,),
            in_specs=specs(own_at) + specs(mate_at),
            out_specs=pl.BlockSpec((tiles, 32, 128), lambda i, *scalars: (0, 0, 0)),
            scratch_shapes=[pltpu.VMEM((9, BLK, 128), jnp.float32)],
        ),
        compiler_params=pltpu.CompilerParams(dimension_semantics=("arbitrary",), vmem_limit_bytes=56000 * 1024),
        name="deposit",
    )(block_tile, block_count, mate_tile, mate_count, corner, offset, radius, emission, extinction, *mate_rest)


def exchange_kernel(rank_ref, partial_ref, image_ref, order_ref, mine, pair, from_up, from_down, via_up, via_down, stack,
                    pair_send, pair_recv, far_send, far_recv, near_send, near_recv, sum_send, sum_recv,
                    stack_send, stack_recv):
    d = lax.axis_index("depth")
    z = lax.axis_index("screen_0")
    core = lax.axis_index("screen_1")
    mate = 1 - core
    y, x = lax.div(d, 4), lax.rem(d, 4)
    z_up, z_down, z_far = lax.rem(z + 1, 4), lax.rem(z + 3, 4), lax.rem(z + 2, 4)
    turns = (2, 1, 3, 0)
    others = [(ry, rx) for ry in turns for rx in (2, 1, 3, 0) if (ry, rx) != (0, 0)]

    def away(ry, rx):
        return lax.rem(y + ry, 4) * 4 + lax.rem(x + rx, 4)

    def row(ry):
        return lax.rem(y + ry, 4) * 4

    barrier = pltpu.get_barrier_semaphore()
    pl.semaphore_signal(barrier, inc=1, device_id={"screen_1": mate}, device_id_type=MESH_ID)
    pl.semaphore_signal(barrier, inc=1, device_id={"screen_0": z_up}, device_id_type=MESH_ID)
    pl.semaphore_signal(barrier, inc=1, device_id={"screen_0": z_down}, device_id_type=MESH_ID)
    for ry, rx in others:
        pl.semaphore_signal(barrier, inc=1, device_id={"depth": away(ry, rx)}, device_id_type=MESH_ID)

    places = (z_far, z_up, z_down, z)

    def pair_copy(p, g):
        rows = pl.ds(row(g), 4)
        return pltpu.make_async_remote_copy(
            partial_ref.at[rows, places[p], mate], pair.at[rows, places[p]],
            pair_send.at[p, g], pair_recv.at[p, g], device_id={"screen_1": mate}, device_id_type=MESH_ID)

    def line_copy(g, half, place, goal, to_up, send, recv):
        rows = pl.ds(row(g) + 2 * half, 2)
        return pltpu.make_async_remote_copy(
            mine.at[rows, place], goal.at[rows], send.at[to_up, g], recv.at[to_up, g],
            device_id={"screen_0": z_up if to_up else z_down}, device_id_type=MESH_ID)

    def far_copy(g, to_up):
        return line_copy(g, 1 - to_up, z_far, via_up if to_up else via_down, to_up, far_send, far_recv)

    def near_copy(g, to_up):
        return line_copy(g, to_up, z_up if to_up else z_down, from_up if to_up else from_down, to_up,
                         near_send, near_recv)

    def sum_copy(g, to_up):
        return line_copy(g, 1 - to_up, z_up if to_up else z_down, from_up if to_up else from_down, to_up,
                         sum_send, sum_recv)

    def stack_copy(ry, rx):
        to = away(ry, rx)
        return pltpu.make_async_remote_copy(
            mine.at[to, z], stack.at[d], stack_send.at[ry, rx], stack_recv.at[ry, rx],
            device_id={"depth": to}, device_id_type=MESH_ID)

    def add_in(first, num, place, terms):
        def one(i, c):
            total = terms[0](first + i)
            for term in terms[1:]:
                total = total + term(first + i)
            mine[first + i, place] = total
            return c
        lax.fori_loop(0, num, one, 0)

    pl.semaphore_wait(barrier, 18)
    for p in range(4):
        for g in turns:
            pair_copy(p, g).start()

    for p in range(16):
        slab = 0
        for j in range(1, 16):
            slab = jnp.where(rank_ref[j] == p, j, slab)
        order_ref[p] = slab

    def take_pair(p, g):
        pair_copy(p, g).wait_recv()

    for g in turns:
        take_pair(0, g)
        add_in(row(g), 4, z_far, [lambda i: partial_ref[i, z_far, core], lambda i: pair[i, z_far]])
        far_copy(g, 1).start()
        far_copy(g, 0).start()
    for g in turns:
        for p, to_up in ((1, 1), (2, 0)):
            take_pair(p, g)
            add_in(row(g), 4, places[p], [lambda i, p=p: partial_ref[i, places[p], core], lambda i, p=p: pair[i, places[p]]])
            near_copy(g, to_up).start()
    for g in turns:
        for to_up in (1, 0):
            far_copy(g, to_up).wait_recv()
            via = via_up if to_up else via_down
            add_in(row(g) + 2 * (1 - to_up), 2, z_up if to_up else z_down, [
                lambda i, to_up=to_up: mine[i, z_up if to_up else z_down], lambda i, via=via: via[i]])
            sum_copy(g, to_up).start()
    for g in turns:
        take_pair(3, g)
        for to_up in (1, 0):
            near_copy(g, to_up).wait_recv()
            sum_copy(g, to_up).wait_recv()
        add_in(row(g), 4, z, [
            lambda i: partial_ref[i, z, core], lambda i: pair[i, z], lambda i: from_up[i], lambda i: from_down[i]])
        for rx in (2, 1, 3, 0):
            if (g, rx) != (0, 0):
                stack_copy(g, rx).start()
    stack[d] = mine[d, z]
    for ry, rx in others:
        stack_copy(ry, rx).wait_recv()

    lane = lax.broadcasted_iota(jnp.int32, (32, 128), 1)

    def one_tile(t, c):
        def one_slab(p, carry):
            prior, light = carry
            value = stack[order_ref[p], t]
            own = jnp.where(lane >= 96, value, 0.0)
            twice = own + pltpu.roll(own, 32, 1)
            optical = twice + pltpu.roll(twice, 64, 1)
            light = light + jnp.exp(-(prior + 0.5 * optical)) * value
            return prior + optical, light
        zero = jnp.zeros((32, 128), jnp.float32)
        prior, light = lax.fori_loop(0, 16, one_slab, (zero, zero), unroll=4)
        image_ref[t] = jnp.where(lane >= 96, 1.0 - jnp.exp(-prior), light)
        return c
    lax.fori_loop(0, 4, one_tile, 0)

    for g in turns:
        for p in range(4):
            pair_copy(p, g).wait_send()
        for to_up in (1, 0):
            far_copy(g, to_up).wait_send()
            near_copy(g, to_up).wait_send()
            sum_copy(g, to_up).wait_send()
    for ry, rx in others:
        stack_copy(ry, rx).wait_send()


def exchange(partial_value, slab_rank):
    dma = pltpu.SemaphoreType.DMA
    return pl.pallas_call(
        exchange_kernel,
        out_shape=jax.ShapeDtypeStruct((4, 32, 128), jnp.float32),
        in_specs=[pl.BlockSpec(memory_space=pltpu.SMEM), pl.BlockSpec(memory_space=pltpu.VMEM)],
        out_specs=pl.BlockSpec(memory_space=pltpu.VMEM),
        scratch_shapes=[
            pltpu.SMEM((16,), jnp.int32),
            pltpu.VMEM((16, 4, 4, 32, 128), jnp.float32),
            pltpu.VMEM((16, 4, 4, 32, 128), jnp.float32),
            pltpu.VMEM((16, 4, 32, 128), jnp.float32),
            pltpu.VMEM((16, 4, 32, 128), jnp.float32),
            pltpu.VMEM((16, 4, 32, 128), jnp.float32),
            pltpu.VMEM((16, 4, 32, 128), jnp.float32),
            pltpu.VMEM((16, 4, 32, 128), jnp.float32),
            dma((4, 4)), dma((4, 4)),
            dma((2, 4)), dma((2, 4)), dma((2, 4)), dma((2, 4)), dma((2, 4)), dma((2, 4)),
            dma((4, 4)), dma((4, 4)),
        ],
        compiler_params=pltpu.CompilerParams(collective_id=0, has_side_effects=True, vmem_limit_bytes=24 * 2**20),
        name="exchange",
    )(slab_rank, partial_value.reshape(16, 4, 2, 4, 32, 128))


def shards(block_tile, block_count, slab_rank, corner, offset, radius, emission, extinction):
    partial_value = deposit_all(
        block_tile, block_count, corner, offset, radius, emission, extinction
    )
    return exchange(partial_value, slab_rank)


def solution(mesh):
    torus = Mesh(mesh.devices.reshape(mesh.shape["depth"], 4, 2), ("depth", "screen_0", "screen_1"))
    placed = (
        P("depth", SCREEN),
        P("depth", SCREEN),
        P(),
        P(None, "depth", SCREEN, None),
        P(None, "depth", SCREEN, None),
        P("depth", SCREEN, None),
        P(None, "depth", SCREEN, None),
        P("depth", SCREEN, None),
    )
    return jax.shard_map(
        shards, mesh=torus, in_specs=placed, out_specs=P(DEPTH_SCREEN, None, None), check_vma=False
    )
```

```python
import functools

import jax
import jax.numpy as jnp
from jax import lax
from jax.experimental import pallas as pl
from jax.experimental.pallas import tpu as pltpu
from jax.sharding import Mesh
from jax.sharding import PartitionSpec as P

SCREEN = ("screen_0", "screen_1")
DEPTH_SCREEN = ("depth", "screen_0", "screen_1")
BLK = 256
UNR = 128

KEPT = 1536
MESH_ID = pl.DeviceIdType.MESH


def share_kernel(tile_ref, count_ref, corner_ref, offset_ref, radius_ref, emission_ref, extinction_ref,
                 tile_out, count_out, corner_out, offset_out, radius_out, emission_out, extinction_out,
                 send_sem, recv_sem):
    mate = 1 - lax.axis_index("screen_1")
    barrier = pltpu.get_barrier_semaphore()
    pl.semaphore_signal(barrier, inc=1, device_id={"screen_1": mate}, device_id_type=MESH_ID)
    pl.semaphore_wait(barrier, 1)
    given = pl.ds(KEPT, tile_ref.shape[1] - KEPT)
    pairs = [
        (tile_ref.at[:, given], tile_out),
        (count_ref, count_out),
        (corner_ref.at[0, :, given], corner_out.at[0]),
        (corner_ref.at[1, :, given], corner_out.at[1]),
        (offset_ref.at[0, :, given], offset_out.at[0]),
        (offset_ref.at[1, :, given], offset_out.at[1]),
        (radius_ref.at[:, given], radius_out),
        (emission_ref.at[0, :, given], emission_out.at[0]),
        (emission_ref.at[1, :, given], emission_out.at[1]),
        (emission_ref.at[2, :, given], emission_out.at[2]),
        (extinction_ref.at[:, given], extinction_out),
    ]
    copies = [
        pltpu.make_async_remote_copy(
            source, goal, send_sem.at[n], recv_sem.at[n], device_id={"screen_1": mate}, device_id_type=MESH_ID)
        for n, (source, goal) in enumerate(pairs)
    ]
    for copy in copies:
        copy.start()
    for copy in copies:
        copy.wait()


def share(block_tile, block_count, corner, offset, radius, emission, extinction):
    num = block_tile.shape[1] - KEPT
    any_spec = pl.BlockSpec(memory_space=pl.ANY)
    def cut(n, dtype):
        return jax.ShapeDtypeStruct((n, 1, num, 128), dtype)
    flat = jax.ShapeDtypeStruct((1, num, 128), jnp.float32)
    return pl.pallas_call(
        share_kernel,
        out_shape=[
            jax.ShapeDtypeStruct((1, num), jnp.int32),
            jax.ShapeDtypeStruct(block_count.shape, jnp.int32),
            cut(2, jnp.int32), cut(2, jnp.float32), flat, cut(3, jnp.float32), flat,
        ],
        in_specs=[any_spec] * 7,
        out_specs=[any_spec] * 7,
        scratch_shapes=[pltpu.SemaphoreType.DMA((11,)), pltpu.SemaphoreType.DMA((11,))],
        compiler_params=pltpu.CompilerParams(collective_id=1, has_side_effects=True),
        name="share",
    )(block_tile, block_count, corner, offset, radius, emission, extinction)


def deposit_kernel(own_steps, tile_ref, count_ref, mate_tile_ref, mate_count_ref, *refs):
    own_refs, mate_refs, (out_ref, pre_ref) = refs[:5], refs[5:10], refs[10:]
    step = pl.program_id(0)
    own = step < own_steps
    first = jnp.minimum(step, own_steps - 1) * BLK
    mate_first = jnp.maximum(step - own_steps, 0) * BLK
    own_live = jnp.minimum(count_ref[0, 0], own_steps * BLK) - first
    mate_live = mate_count_ref[0, 0] - own_steps * BLK - mate_first
    live_num = jnp.where(own, own_live, mate_live)

    @pl.when(step == 0)
    def _():
        def zero(t, c):
            out_ref[t] = jnp.zeros(out_ref.shape[1:], jnp.float32)
            return c
        lax.fori_loop(0, out_ref.shape[0], zero, 0, unroll=8)

    def prepare(corner_ref, offset_ref, radius_ref, emission_ref, extinction_ref):
        live = lax.broadcasted_iota(jnp.int32, (BLK, 128), 0) < live_num
        radius = radius_ref[0]
        h2 = radius * radius
        h4 = h2 * h2
        scale = jnp.where(live, 1.0 / (h4 * h4), 0.0)
        for k in range(2):
            edge = corner_ref[k, 0].astype(jnp.float32)
            pre_ref[2 * k] = edge
            pre_ref[2 * k + 1] = edge + 16.0 * offset_ref[k, 0] - 0.5
        pre_ref[4] = h2
        for c in range(3):
            pre_ref[5 + c] = emission_ref[c, 0] * scale
        pre_ref[8] = extinction_ref[0] * scale

    @pl.when(jnp.logical_and(own, live_num > 0))
    def _():
        prepare(*own_refs)

    @pl.when(jnp.logical_and(jnp.logical_not(own), live_num > 0))
    def _():
        prepare(*mate_refs)

    @pl.when(live_num > 0)
    def _():
        rows = lax.broadcasted_iota(jnp.int32, (16, 128), 0).astype(jnp.float32)
        rows16 = rows.astype(jnp.bfloat16)
        zero16 = jnp.zeros((16, 128), jnp.bfloat16)

        def split(w):
            high = w.astype(jnp.bfloat16)
            low = (w - high.astype(jnp.float32)).astype(jnp.bfloat16)
            return high, low

        def one_group(g, c):
            outs = []
            for u in range(UNR):
                j = g * UNR + u
                def row(a):
                    return jnp.broadcast_to(pre_ref[a, pl.ds(j, 1), :], (16, 128))
                h2r = row(4)
                def bump(k):
                    edge = row(2 * k)
                    mask16 = rows16 < edge.astype(jnp.bfloat16)
                    at = jnp.where(rows < edge, rows + 16.0, rows)
                    s = at - row(2 * k + 1)
                    v = jnp.maximum(h2r - s * s, 0.0)
                    return v * v, mask16
                wx, mx = bump(0)
                wy, my = bump(1)
                def spread(w16, m):
                    return [jnp.where(m, zero16, w16), jnp.where(m, w16, zero16)]
                yh, yl = split(wy)
                lhs = jnp.concatenate(spread(yh, my) + spread(yl, my), 0)
                lhs = jnp.concatenate([lhs, lhs], 1)
                hi, lo = [], []
                for ch in range(4):
                    a, b = split(row(5 + ch) * wx)
                    hi += spread(a, mx)
                    lo += spread(b, mx)
                rhs = jnp.concatenate([jnp.concatenate(hi, 0), jnp.concatenate(lo, 0)], 1)
                outs.append(lax.dot_general(lhs, rhs, (((1,), (1,)), ((), ())), preferred_element_type=jnp.float32))
            for u in range(UNR):
                t = jnp.where(own, tile_ref[0, first + g * UNR + u], mate_tile_ref[0, mate_first + g * UNR + u])
                out_ref[t] += outs[u][:32] + outs[u][32:]
            return c

        groups = lax.div(jnp.minimum(live_num, BLK) + (UNR - 1), UNR)
        lax.fori_loop(0, groups, one_group, 0)


def deposit_all(block_tile, block_count, corner, offset, radius, emission, extinction, tiles=512):
    mate_tile, mate_count, *mate_rest = share(block_tile, block_count, corner, offset, radius, emission, extinction)
    own_steps = KEPT // BLK
    steps = block_tile.shape[1] // BLK
    def own_at(i, tile, count, *unused):
        return jnp.minimum(jnp.minimum(i, own_steps - 1), lax.div(count[0, 0] - 1, BLK))
    def mate_at(i, *unused):
        return jnp.maximum(i - own_steps, 0)
    def specs(at):
        def m4(n):
            return pl.BlockSpec((n, 1, BLK, 128), lambda i, *scalars: (0, 0, at(i, *scalars), 0))
        def m3():
            return pl.BlockSpec((1, BLK, 128), lambda i, *scalars: (0, at(i, *scalars), 0))
        return [m4(2), m4(2), m3(), m4(3), m3()]
    return pl.pallas_call(
        functools.partial(deposit_kernel, own_steps),
        out_shape=pltpu.VMEM((tiles, 32, 128), jnp.float32),
        grid_spec=pltpu.PrefetchScalarGridSpec(
            num_scalar_prefetch=4, grid=(steps,),
            in_specs=specs(own_at) + specs(mate_at),
            out_specs=pl.BlockSpec((tiles, 32, 128), lambda i, *scalars: (0, 0, 0)),
            scratch_shapes=[pltpu.VMEM((9, BLK, 128), jnp.float32)],
        ),
        compiler_params=pltpu.CompilerParams(dimension_semantics=("arbitrary",), vmem_limit_bytes=56000 * 1024),
        name="deposit",
    )(block_tile, block_count, mate_tile, mate_count, corner, offset, radius, emission, extinction, *mate_rest)


def exchange_kernel(rank_ref, partial_ref, image_ref, order_ref, mine, pair, from_up, from_down, via_up, via_down, stack,
                    pair_send, pair_recv, far_send, far_recv, near_send, near_recv, sum_send, sum_recv,
                    stack_send, stack_recv):
    d = lax.axis_index("depth")
    z = lax.axis_index("screen_0")
    core = lax.axis_index("screen_1")
    mate = 1 - core
    y, x = lax.div(d, 4), lax.rem(d, 4)
    z_up, z_down, z_far = lax.rem(z + 1, 4), lax.rem(z + 3, 4), lax.rem(z + 2, 4)
    turns = (2, 1, 3, 0)
    steps = (2, 3, 1, 0)
    summed_up = (2, 1)
    others = [(ry, rx) for ry in turns for rx in (2, 1, 3, 0) if (ry, rx) != (0, 0)]

    def away(ry, rx):
        return lax.rem(y + ry, 4) * 4 + lax.rem(x + rx, 4)

    def row(ry):
        return lax.rem(y + ry, 4) * 4

    barrier = pltpu.get_barrier_semaphore()
    pl.semaphore_signal(barrier, inc=1, device_id={"screen_1": mate}, device_id_type=MESH_ID)
    pl.semaphore_signal(barrier, inc=1, device_id={"screen_0": z_up}, device_id_type=MESH_ID)
    pl.semaphore_signal(barrier, inc=1, device_id={"screen_0": z_down}, device_id_type=MESH_ID)
    for ry, rx in others:
        pl.semaphore_signal(barrier, inc=1, device_id={"depth": away(ry, rx)}, device_id_type=MESH_ID)

    places = (z_far, z_up, z_down, z)

    def pair_copy(p, g):
        rows = pl.ds(row(g), 4)
        return pltpu.make_async_remote_copy(
            partial_ref.at[rows, places[p], mate], pair.at[rows, places[p]],
            pair_send.at[p, g], pair_recv.at[p, g], device_id={"screen_1": mate}, device_id_type=MESH_ID)

    def line_copy(ry, rx, place, goal, to_up, send, recv):
        to, n = away(ry, rx), (2, 1, 3, 0).index(rx) % 2
        return pltpu.make_async_remote_copy(
            mine.at[to, place], goal.at[to], send.at[to_up, ry, n], recv.at[to_up, ry, n],
            device_id={"screen_0": z_up if to_up else z_down}, device_id_type=MESH_ID)

    def far_copy(ry, rx):
        to_up = int(rx in summed_up)
        return line_copy(ry, rx, z_far, via_up if to_up else via_down, to_up, far_send, far_recv)

    def near_copy(ry, rx):
        to_up = int(rx not in summed_up)
        return line_copy(ry, rx, z_up if to_up else z_down, from_up if to_up else from_down, to_up,
                         near_send, near_recv)

    def sum_copy(ry, rx):
        to_up = int(rx in summed_up)
        return line_copy(ry, rx, z_up if to_up else z_down, from_up if to_up else from_down, to_up,
                         sum_send, sum_recv)

    def stack_copy(ry, rx):
        to = away(ry, rx)
        return pltpu.make_async_remote_copy(
            mine.at[to, z], stack.at[d], stack_send.at[ry, rx], stack_recv.at[ry, rx],
            device_id={"depth": to}, device_id_type=MESH_ID)

    def add_in(first, num, place, terms):
        def one(i, c):
            total = terms[0](first + i)
            for term in terms[1:]:
                total = total + term(first + i)
            mine[first + i, place] = total
            return c
        lax.fori_loop(0, num, one, 0)

    pl.semaphore_wait(barrier, 18)
    for p in range(4):
        for g in turns:
            pair_copy(p, g).start()

    for p in range(16):
        slab = 0
        for j in range(1, 16):
            slab = jnp.where(rank_ref[j] == p, j, slab)
        order_ref[p] = slab

    def take_pair(p, g):
        pair_copy(p, g).wait_recv()

    for g in turns:
        take_pair(0, g)
        add_in(row(g), 4, z_far, [lambda i: partial_ref[i, z_far, core], lambda i: pair[i, z_far]])
        for rx in steps:
            far_copy(g, rx).start()
    for g in turns:
        for p, to_up in ((1, 1), (2, 0)):
            take_pair(p, g)
            add_in(row(g), 4, places[p], [
                lambda i, p=p: partial_ref[i, places[p], core], lambda i, p=p: pair[i, places[p]]])
            for rx in steps:
                if int(rx not in summed_up) == to_up:
                    near_copy(g, rx).start()
    for g in turns:
        for rx in steps:
            far_copy(g, rx).wait_recv()
            to_up = int(rx in summed_up)
            via, place = (via_up, z_up) if to_up else (via_down, z_down)
            add_in(away(g, rx), 1, place, [
                lambda i, place=place: mine[i, place], lambda i, via=via: via[i]])
            sum_copy(g, rx).start()
    for g in turns:
        take_pair(3, g)
        for rx in steps:
            near_copy(g, rx).wait_recv()
            sum_copy(g, rx).wait_recv()
            add_in(away(g, rx), 1, z, [
                lambda i: partial_ref[i, z, core], lambda i: pair[i, z], lambda i: from_up[i], lambda i: from_down[i]])
            if (g, rx) != (0, 0):
                stack_copy(g, rx).start()
    stack[d] = mine[d, z]
    for ry, rx in others:
        stack_copy(ry, rx).wait_recv()

    lane = lax.broadcasted_iota(jnp.int32, (2, 32, 128), 2)

    for t in (0, 2):
        def one_slab(p, carry, t=t):
            prior, light = carry
            value = stack[order_ref[p], pl.ds(t, 2)]
            own = jnp.where(lane >= 96, value, 0.0)
            twice = own + pltpu.roll(own, 32, 2)
            optical = twice + pltpu.roll(twice, 64, 2)
            light = light + jnp.exp(-(prior + 0.5 * optical)) * value
            return prior + optical, light
        zero = jnp.zeros((2, 32, 128), jnp.float32)
        prior, light = lax.fori_loop(0, 16, one_slab, (zero, zero), unroll=4)
        image_ref[pl.ds(t, 2)] = jnp.where(lane >= 96, 1.0 - jnp.exp(-prior), light)

    for g in turns:
        for p in range(4):
            pair_copy(p, g).wait_send()
        for rx in steps:
            far_copy(g, rx).wait_send()
            near_copy(g, rx).wait_send()
            sum_copy(g, rx).wait_send()
    for ry, rx in others:
        stack_copy(ry, rx).wait_send()


def exchange(partial_value, slab_rank):
    dma = pltpu.SemaphoreType.DMA
    return pl.pallas_call(
        exchange_kernel,
        out_shape=jax.ShapeDtypeStruct((4, 32, 128), jnp.float32),
        in_specs=[pl.BlockSpec(memory_space=pltpu.SMEM), pl.BlockSpec(memory_space=pltpu.VMEM)],
        out_specs=pl.BlockSpec(memory_space=pltpu.VMEM),
        scratch_shapes=[
            pltpu.SMEM((16,), jnp.int32),
            pltpu.VMEM((16, 4, 4, 32, 128), jnp.float32),
            pltpu.VMEM((16, 4, 4, 32, 128), jnp.float32),
            pltpu.VMEM((16, 4, 32, 128), jnp.float32),
            pltpu.VMEM((16, 4, 32, 128), jnp.float32),
            pltpu.VMEM((16, 4, 32, 128), jnp.float32),
            pltpu.VMEM((16, 4, 32, 128), jnp.float32),
            pltpu.VMEM((16, 4, 32, 128), jnp.float32),
            dma((4, 4)), dma((4, 4)),
            *[dma((2, 4, 2))] * 6,
            dma((4, 4)), dma((4, 4)),
        ],
        compiler_params=pltpu.CompilerParams(collective_id=0, has_side_effects=True, vmem_limit_bytes=24 * 2**20),
        name="exchange",
    )(slab_rank, partial_value.reshape(16, 4, 2, 4, 32, 128))


def shards(block_tile, block_count, slab_rank, corner, offset, radius, emission, extinction):
    partial_value = deposit_all(
        block_tile, block_count, corner, offset, radius, emission, extinction
    )
    return exchange(partial_value, slab_rank)


def solution(mesh):
    torus = Mesh(mesh.devices.reshape(mesh.shape["depth"], 4, 2), ("depth", "screen_0", "screen_1"))
    placed = (
        P("depth", SCREEN),
        P("depth", SCREEN),
        P(),
        P(None, "depth", SCREEN, None),
        P(None, "depth", SCREEN, None),
        P("depth", SCREEN, None),
        P(None, "depth", SCREEN, None),
        P("depth", SCREEN, None),
    )
    return jax.shard_map(
        shards, mesh=torus, in_specs=placed, out_specs=P(DEPTH_SCREEN, None, None), check_vma=False
    )
```

```python
import functools

import jax
import jax.numpy as jnp
from jax import lax
from jax.experimental import pallas as pl
from jax.experimental.pallas import tpu as pltpu
from jax.sharding import Mesh
from jax.sharding import PartitionSpec as P

SCREEN = ("screen_0", "screen_1")
DEPTH_SCREEN = ("depth", "screen_0", "screen_1")
BLK = 256
UNR = 256

KEPT = 1536
MESH_ID = pl.DeviceIdType.MESH


def share_kernel(tile_ref, count_ref, corner_ref, offset_ref, radius_ref, emission_ref, extinction_ref,
                 tile_out, count_out, corner_out, offset_out, radius_out, emission_out, extinction_out,
                 send_sem, recv_sem):
    mate = 1 - lax.axis_index("screen_1")
    barrier = pltpu.get_barrier_semaphore()
    pl.semaphore_signal(barrier, inc=1, device_id={"screen_1": mate}, device_id_type=MESH_ID)
    pl.semaphore_wait(barrier, 1)
    given = pl.ds(KEPT, tile_ref.shape[1] - KEPT)
    pairs = [
        (tile_ref.at[:, given], tile_out),
        (count_ref, count_out),
        (corner_ref.at[0, :, given], corner_out.at[0]),
        (corner_ref.at[1, :, given], corner_out.at[1]),
        (offset_ref.at[0, :, given], offset_out.at[0]),
        (offset_ref.at[1, :, given], offset_out.at[1]),
        (radius_ref.at[:, given], radius_out),
        (emission_ref.at[0, :, given], emission_out.at[0]),
        (emission_ref.at[1, :, given], emission_out.at[1]),
        (emission_ref.at[2, :, given], emission_out.at[2]),
        (extinction_ref.at[:, given], extinction_out),
    ]
    copies = [
        pltpu.make_async_remote_copy(
            source, goal, send_sem.at[n], recv_sem.at[n], device_id={"screen_1": mate}, device_id_type=MESH_ID)
        for n, (source, goal) in enumerate(pairs)
    ]
    for copy in copies:
        copy.start()
    for copy in copies:
        copy.wait()


def share(block_tile, block_count, corner, offset, radius, emission, extinction):
    num = block_tile.shape[1] - KEPT
    any_spec = pl.BlockSpec(memory_space=pl.ANY)
    def cut(n, dtype):
        return jax.ShapeDtypeStruct((n, 1, num, 128), dtype)
    flat = jax.ShapeDtypeStruct((1, num, 128), jnp.float32)
    return pl.pallas_call(
        share_kernel,
        out_shape=[
            jax.ShapeDtypeStruct((1, num), jnp.int32),
            jax.ShapeDtypeStruct(block_count.shape, jnp.int32),
            cut(2, jnp.int32), cut(2, jnp.float32), flat, cut(3, jnp.float32), flat,
        ],
        in_specs=[any_spec] * 7,
        out_specs=[any_spec] * 7,
        scratch_shapes=[pltpu.SemaphoreType.DMA((11,)), pltpu.SemaphoreType.DMA((11,))],
        compiler_params=pltpu.CompilerParams(collective_id=1, has_side_effects=True),
        name="share",
    )(block_tile, block_count, corner, offset, radius, emission, extinction)


def deposit_kernel(own_steps, tile_ref, count_ref, mate_tile_ref, mate_count_ref, *refs):
    own_refs, mate_refs, (out_ref, pre_ref) = refs[:5], refs[5:10], refs[10:]
    step = pl.program_id(0)
    own = step < own_steps
    first = jnp.minimum(step, own_steps - 1) * BLK
    mate_first = jnp.maximum(step - own_steps, 0) * BLK
    own_live = jnp.minimum(count_ref[0, 0], own_steps * BLK) - first
    mate_live = mate_count_ref[0, 0] - own_steps * BLK - mate_first
    live_num = jnp.where(own, own_live, mate_live)

    @pl.when(step == 0)
    def _():
        def zero(t, c):
            out_ref[t] = jnp.zeros(out_ref.shape[1:], jnp.float32)
            return c
        lax.fori_loop(0, out_ref.shape[0], zero, 0, unroll=8)

    def prepare(corner_ref, offset_ref, radius_ref, emission_ref, extinction_ref):
        live = lax.broadcasted_iota(jnp.int32, (BLK, 128), 0) < live_num
        radius = radius_ref[0]
        h2 = radius * radius
        h4 = h2 * h2
        scale = jnp.where(live, 1.0 / (h4 * h4), 0.0)
        for k in range(2):
            edge = corner_ref[k, 0].astype(jnp.float32)
            pre_ref[2 * k] = edge
            pre_ref[2 * k + 1] = edge + 16.0 * offset_ref[k, 0] - 0.5
        pre_ref[4] = h2
        for c in range(3):
            pre_ref[5 + c] = emission_ref[c, 0] * scale
        pre_ref[8] = extinction_ref[0] * scale

    @pl.when(jnp.logical_and(own, live_num > 0))
    def _():
        prepare(*own_refs)

    @pl.when(jnp.logical_and(jnp.logical_not(own), live_num > 0))
    def _():
        prepare(*mate_refs)

    @pl.when(live_num > 0)
    def _():
        rows = lax.broadcasted_iota(jnp.int32, (16, 128), 0).astype(jnp.float32)
        rows16 = rows.astype(jnp.bfloat16)
        zero16 = jnp.zeros((16, 128), jnp.bfloat16)

        def split(w):
            high = w.astype(jnp.bfloat16)
            low = (w - high.astype(jnp.float32)).astype(jnp.bfloat16)
            return high, low

        def one_group(g, c):
            outs = []
            for u in range(UNR):
                j = g * UNR + u
                def row(a):
                    return jnp.broadcast_to(pre_ref[a, pl.ds(j, 1), :], (16, 128))
                h2r = row(4)
                def bump(k):
                    edge = row(2 * k)
                    mask16 = rows16 < edge.astype(jnp.bfloat16)
                    at = jnp.where(rows < edge, rows + 16.0, rows)
                    s = at - row(2 * k + 1)
                    v = jnp.maximum(h2r - s * s, 0.0)
                    return v * v, mask16
                wx, mx = bump(0)
                wy, my = bump(1)
                def spread(w16, m):
                    return [jnp.where(m, zero16, w16), jnp.where(m, w16, zero16)]
                yh, yl = split(wy)
                lhs = jnp.concatenate(spread(yh, my) + spread(yl, my), 0)
                lhs = jnp.concatenate([lhs, lhs], 1)
                hi, lo = [], []
                for ch in range(4):
                    a, b = split(row(5 + ch) * wx)
                    hi += spread(a, mx)
                    lo += spread(b, mx)
                rhs = jnp.concatenate([jnp.concatenate(hi, 0), jnp.concatenate(lo, 0)], 1)
                outs.append(lax.dot_general(lhs, rhs, (((1,), (1,)), ((), ())), preferred_element_type=jnp.float32))
            for u in range(UNR):
                t = jnp.where(own, tile_ref[0, first + g * UNR + u], mate_tile_ref[0, mate_first + g * UNR + u])
                out_ref[t] += outs[u][:32] + outs[u][32:]
            return c

        groups = lax.div(jnp.minimum(live_num, BLK) + (UNR - 1), UNR)
        lax.fori_loop(0, groups, one_group, 0)


def deposit_all(block_tile, block_count, corner, offset, radius, emission, extinction, tiles=512):
    mate_tile, mate_count, *mate_rest = share(block_tile, block_count, corner, offset, radius, emission, extinction)
    own_steps = KEPT // BLK
    steps = block_tile.shape[1] // BLK
    def own_at(i, tile, count, *unused):
        return jnp.minimum(jnp.minimum(i, own_steps - 1), lax.div(count[0, 0] - 1, BLK))
    def mate_at(i, *unused):
        return jnp.maximum(i - own_steps, 0)
    def specs(at):
        def m4(n):
            return pl.BlockSpec((n, 1, BLK, 128), lambda i, *scalars: (0, 0, at(i, *scalars), 0))
        def m3():
            return pl.BlockSpec((1, BLK, 128), lambda i, *scalars: (0, at(i, *scalars), 0))
        return [m4(2), m4(2), m3(), m4(3), m3()]
    return pl.pallas_call(
        functools.partial(deposit_kernel, own_steps),
        out_shape=pltpu.VMEM((tiles, 32, 128), jnp.float32),
        grid_spec=pltpu.PrefetchScalarGridSpec(
            num_scalar_prefetch=4, grid=(steps,),
            in_specs=specs(own_at) + specs(mate_at),
            out_specs=pl.BlockSpec((tiles, 32, 128), lambda i, *scalars: (0, 0, 0)),
            scratch_shapes=[pltpu.VMEM((9, BLK, 128), jnp.float32)],
        ),
        compiler_params=pltpu.CompilerParams(dimension_semantics=("arbitrary",), vmem_limit_bytes=56000 * 1024),
        name="deposit",
    )(block_tile, block_count, mate_tile, mate_count, corner, offset, radius, emission, extinction, *mate_rest)


def exchange_kernel(rank_ref, partial_ref, image_ref, order_ref, mine, pair, from_up, from_down, via_up, via_down, stack,
                    pair_send, pair_recv, far_send, far_recv, near_send, near_recv, sum_send, sum_recv,
                    stack_send, stack_recv):
    d = lax.axis_index("depth")
    z = lax.axis_index("screen_0")
    core = lax.axis_index("screen_1")
    mate = 1 - core
    y, x = lax.div(d, 4), lax.rem(d, 4)
    z_up, z_down, z_far = lax.rem(z + 1, 4), lax.rem(z + 3, 4), lax.rem(z + 2, 4)
    turns = (2, 1, 3, 0)
    steps = (2, 3, 1, 0)
    summed_up = (2, 1)
    others = [(ry, rx) for ry in turns for rx in (2, 1, 3, 0) if (ry, rx) != (0, 0)]

    def away(ry, rx):
        return lax.rem(y + ry, 4) * 4 + lax.rem(x + rx, 4)

    def row(ry):
        return lax.rem(y + ry, 4) * 4

    barrier = pltpu.get_barrier_semaphore()
    pl.semaphore_signal(barrier, inc=1, device_id={"screen_1": mate}, device_id_type=MESH_ID)
    pl.semaphore_signal(barrier, inc=1, device_id={"screen_0": z_up}, device_id_type=MESH_ID)
    pl.semaphore_signal(barrier, inc=1, device_id={"screen_0": z_down}, device_id_type=MESH_ID)
    for ry, rx in others:
        pl.semaphore_signal(barrier, inc=1, device_id={"depth": away(ry, rx)}, device_id_type=MESH_ID)

    places = (z_far, z_up, z_down, z)

    def pair_copy(p, g):
        rows = pl.ds(row(g), 4)
        return pltpu.make_async_remote_copy(
            partial_ref.at[rows, places[p], mate], pair.at[rows, places[p]],
            pair_send.at[p, g], pair_recv.at[p, g], device_id={"screen_1": mate}, device_id_type=MESH_ID)

    def line_copy(ry, rx, place, goal, to_up, send, recv):
        to, n = away(ry, rx), (2, 1, 3, 0).index(rx) % 2
        return pltpu.make_async_remote_copy(
            mine.at[to, place], goal.at[to], send.at[to_up, ry, n], recv.at[to_up, ry, n],
            device_id={"screen_0": z_up if to_up else z_down}, device_id_type=MESH_ID)

    def far_copy(ry, rx):
        to_up = int(rx in summed_up)
        return line_copy(ry, rx, z_far, via_up if to_up else via_down, to_up, far_send, far_recv)

    def near_copy(ry, rx):
        to_up = int(rx not in summed_up)
        return line_copy(ry, rx, z_up if to_up else z_down, from_up if to_up else from_down, to_up,
                         near_send, near_recv)

    def sum_copy(ry, rx):
        to_up = int(rx in summed_up)
        return line_copy(ry, rx, z_up if to_up else z_down, from_up if to_up else from_down, to_up,
                         sum_send, sum_recv)

    def stack_copy(ry, rx):
        to = away(ry, rx)
        return pltpu.make_async_remote_copy(
            mine.at[to, z], stack.at[d], stack_send.at[ry, rx], stack_recv.at[ry, rx],
            device_id={"depth": to}, device_id_type=MESH_ID)

    def add_in(first, num, place, terms):
        def one(i, c):
            total = terms[0](first + i)
            for term in terms[1:]:
                total = total + term(first + i)
            mine[first + i, place] = total
            return c
        lax.fori_loop(0, num, one, 0)

    pl.semaphore_wait(barrier, 18)
    for p in range(4):
        for g in turns:
            pair_copy(p, g).start()

    for p in range(16):
        slab = 0
        for j in range(1, 16):
            slab = jnp.where(rank_ref[j] == p, j, slab)
        order_ref[p] = slab

    def take_pair(p, g):
        pair_copy(p, g).wait_recv()

    for g in turns:
        take_pair(0, g)
        add_in(row(g), 4, z_far, [lambda i: partial_ref[i, z_far, core], lambda i: pair[i, z_far]])
        for rx in steps:
            far_copy(g, rx).start()
    for g in turns:
        for p, to_up in ((1, 1), (2, 0)):
            take_pair(p, g)
            add_in(row(g), 4, places[p], [
                lambda i, p=p: partial_ref[i, places[p], core], lambda i, p=p: pair[i, places[p]]])
            for rx in steps:
                if int(rx not in summed_up) == to_up:
                    near_copy(g, rx).start()
    for g in turns:
        for rx in steps:
            far_copy(g, rx).wait_recv()
            to_up = int(rx in summed_up)
            via, place = (via_up, z_up) if to_up else (via_down, z_down)
            add_in(away(g, rx), 1, place, [
                lambda i, place=place: mine[i, place], lambda i, via=via: via[i]])
            sum_copy(g, rx).start()
    for g in turns:
        take_pair(3, g)
        for rx in steps:
            near_copy(g, rx).wait_recv()
            sum_copy(g, rx).wait_recv()
            add_in(away(g, rx), 1, z, [
                lambda i: partial_ref[i, z, core], lambda i: pair[i, z], lambda i: from_up[i], lambda i: from_down[i]])
            if (g, rx) != (0, 0):
                stack_copy(g, rx).start()
    stack[d] = mine[d, z]
    for ry, rx in others:
        stack_copy(ry, rx).wait_recv()

    lane = lax.broadcasted_iota(jnp.int32, (2, 32, 128), 2)

    for t in (0, 2):
        def one_slab(p, carry, t=t):
            prior, light = carry
            value = stack[order_ref[p], pl.ds(t, 2)]
            own = jnp.where(lane >= 96, value, 0.0)
            twice = own + pltpu.roll(own, 32, 2)
            optical = twice + pltpu.roll(twice, 64, 2)
            light = light + jnp.exp(-(prior + 0.5 * optical)) * value
            return prior + optical, light
        zero = jnp.zeros((2, 32, 128), jnp.float32)
        prior, light = lax.fori_loop(0, 16, one_slab, (zero, zero), unroll=4)
        image_ref[pl.ds(t, 2)] = jnp.where(lane >= 96, 1.0 - jnp.exp(-prior), light)

    for g in turns:
        for p in range(4):
            pair_copy(p, g).wait_send()
        for rx in steps:
            far_copy(g, rx).wait_send()
            near_copy(g, rx).wait_send()
            sum_copy(g, rx).wait_send()
    for ry, rx in others:
        stack_copy(ry, rx).wait_send()


def exchange(partial_value, slab_rank):
    dma = pltpu.SemaphoreType.DMA
    return pl.pallas_call(
        exchange_kernel,
        out_shape=jax.ShapeDtypeStruct((4, 32, 128), jnp.float32),
        in_specs=[pl.BlockSpec(memory_space=pltpu.SMEM), pl.BlockSpec(memory_space=pltpu.VMEM)],
        out_specs=pl.BlockSpec(memory_space=pltpu.VMEM),
        scratch_shapes=[
            pltpu.SMEM((16,), jnp.int32),
            pltpu.VMEM((16, 4, 4, 32, 128), jnp.float32),
            pltpu.VMEM((16, 4, 4, 32, 128), jnp.float32),
            pltpu.VMEM((16, 4, 32, 128), jnp.float32),
            pltpu.VMEM((16, 4, 32, 128), jnp.float32),
            pltpu.VMEM((16, 4, 32, 128), jnp.float32),
            pltpu.VMEM((16, 4, 32, 128), jnp.float32),
            pltpu.VMEM((16, 4, 32, 128), jnp.float32),
            dma((4, 4)), dma((4, 4)),
            *[dma((2, 4, 2))] * 6,
            dma((4, 4)), dma((4, 4)),
        ],
        compiler_params=pltpu.CompilerParams(collective_id=0, has_side_effects=True, vmem_limit_bytes=24 * 2**20),
        name="exchange",
    )(slab_rank, partial_value.reshape(16, 4, 2, 4, 32, 128))


def shards(block_tile, block_count, slab_rank, corner, offset, radius, emission, extinction):
    partial_value = deposit_all(
        block_tile, block_count, corner, offset, radius, emission, extinction
    )
    return exchange(partial_value, slab_rank)


def solution(mesh):
    torus = Mesh(mesh.devices.reshape(mesh.shape["depth"], 4, 2), ("depth", "screen_0", "screen_1"))
    placed = (
        P("depth", SCREEN),
        P("depth", SCREEN),
        P(),
        P(None, "depth", SCREEN, None),
        P(None, "depth", SCREEN, None),
        P("depth", SCREEN, None),
        P(None, "depth", SCREEN, None),
        P("depth", SCREEN, None),
    )
    return jax.shard_map(
        shards, mesh=torus, in_specs=placed, out_specs=P(DEPTH_SCREEN, None, None), check_vma=False
    )
```

```python
import functools

import jax
import jax.numpy as jnp
from jax import lax
from jax.experimental import pallas as pl
from jax.experimental.pallas import tpu as pltpu
from jax.sharding import Mesh
from jax.sharding import PartitionSpec as P

SCREEN = ("screen_0", "screen_1")
DEPTH_SCREEN = ("depth", "screen_0", "screen_1")
BLK = 256
UNR = 256

KEPT = 1536
MESH_ID = pl.DeviceIdType.MESH


def share_kernel(tile_ref, count_ref, corner_ref, offset_ref, radius_ref, emission_ref, extinction_ref,
                 tile_out, count_out, corner_out, offset_out, radius_out, emission_out, extinction_out,
                 send_sem, recv_sem):
    mate = 1 - lax.axis_index("screen_1")
    barrier = pltpu.get_barrier_semaphore()
    pl.semaphore_signal(barrier, inc=1, device_id={"screen_1": mate}, device_id_type=MESH_ID)
    pl.semaphore_wait(barrier, 1)
    given = pl.ds(KEPT, tile_ref.shape[1] - KEPT)
    pairs = [
        (tile_ref.at[:, given], tile_out),
        (count_ref, count_out),
        (corner_ref.at[0, :, given], corner_out.at[0]),
        (corner_ref.at[1, :, given], corner_out.at[1]),
        (offset_ref.at[0, :, given], offset_out.at[0]),
        (offset_ref.at[1, :, given], offset_out.at[1]),
        (radius_ref.at[:, given], radius_out),
        (emission_ref.at[0, :, given], emission_out.at[0]),
        (emission_ref.at[1, :, given], emission_out.at[1]),
        (emission_ref.at[2, :, given], emission_out.at[2]),
        (extinction_ref.at[:, given], extinction_out),
    ]
    copies = [
        pltpu.make_async_remote_copy(
            source, goal, send_sem.at[n], recv_sem.at[n], device_id={"screen_1": mate}, device_id_type=MESH_ID)
        for n, (source, goal) in enumerate(pairs)
    ]
    for copy in copies:
        copy.start()
    for copy in copies:
        copy.wait()


def share(block_tile, block_count, corner, offset, radius, emission, extinction):
    num = block_tile.shape[1] - KEPT
    any_spec = pl.BlockSpec(memory_space=pl.ANY)
    def cut(n, dtype):
        return jax.ShapeDtypeStruct((n, 1, num, 128), dtype)
    flat = jax.ShapeDtypeStruct((1, num, 128), jnp.float32)
    return pl.pallas_call(
        share_kernel,
        out_shape=[
            jax.ShapeDtypeStruct((1, num), jnp.int32),
            jax.ShapeDtypeStruct(block_count.shape, jnp.int32),
            cut(2, jnp.int32), cut(2, jnp.float32), flat, cut(3, jnp.float32), flat,
        ],
        in_specs=[any_spec] * 7,
        out_specs=[any_spec] * 7,
        scratch_shapes=[pltpu.SemaphoreType.DMA((11,)), pltpu.SemaphoreType.DMA((11,))],
        compiler_params=pltpu.CompilerParams(collective_id=1, has_side_effects=True),
        name="share",
    )(block_tile, block_count, corner, offset, radius, emission, extinction)


def deposit_kernel(own_steps, tile_ref, count_ref, mate_tile_ref, mate_count_ref, *refs):
    own_refs, mate_refs, (out_ref, pre_ref) = refs[:5], refs[5:10], refs[10:]
    step = pl.program_id(0)
    own = step < own_steps
    first = jnp.minimum(step, own_steps - 1) * BLK
    mate_first = jnp.maximum(step - own_steps, 0) * BLK
    own_live = jnp.minimum(count_ref[0, 0], own_steps * BLK) - first
    mate_live = mate_count_ref[0, 0] - own_steps * BLK - mate_first
    live_num = jnp.where(own, own_live, mate_live)

    @pl.when(step == 0)
    def _():
        def zero(t, c):
            out_ref[t] = jnp.zeros(out_ref.shape[1:], jnp.float32)
            return c
        lax.fori_loop(0, out_ref.shape[0], zero, 0, unroll=8)

    def prepare(corner_ref, offset_ref, radius_ref, emission_ref, extinction_ref):
        live = lax.broadcasted_iota(jnp.int32, (BLK, 128), 0) < live_num
        radius = radius_ref[0]
        h2 = radius * radius
        h4 = h2 * h2
        scale = jnp.where(live, 1.0 / (h4 * h4), 0.0)
        for k in range(2):
            edge = corner_ref[k, 0].astype(jnp.float32)
            pre_ref[2 * k] = edge
            pre_ref[2 * k + 1] = edge + 16.0 * offset_ref[k, 0] - 0.5
        pre_ref[4] = h2
        for c in range(3):
            pre_ref[5 + c] = emission_ref[c, 0] * scale
        pre_ref[8] = extinction_ref[0] * scale

    @pl.when(jnp.logical_and(own, live_num > 0))
    def _():
        prepare(*own_refs)

    @pl.when(jnp.logical_and(jnp.logical_not(own), live_num > 0))
    def _():
        prepare(*mate_refs)

    @pl.when(live_num > 0)
    def _():
        rows = lax.broadcasted_iota(jnp.int32, (16, 128), 0).astype(jnp.float32)
        rows16 = rows.astype(jnp.bfloat16)
        zero16 = jnp.zeros((16, 128), jnp.bfloat16)

        def split(w):
            high = w.astype(jnp.bfloat16)
            low = (w - high.astype(jnp.float32)).astype(jnp.bfloat16)
            return high, low

        def one_group(g, c):
            outs = []
            for u in range(UNR):
                j = g * UNR + u
                def row(a):
                    return jnp.broadcast_to(pre_ref[a, pl.ds(j, 1), :], (16, 128))
                h2r = row(4)
                def bump(k):
                    edge = row(2 * k)
                    mask16 = rows16 < edge.astype(jnp.bfloat16)
                    at = jnp.where(rows < edge, rows + 16.0, rows)
                    s = at - row(2 * k + 1)
                    v = jnp.maximum(h2r - s * s, 0.0)
                    return v * v, mask16
                wx, mx = bump(0)
                wy, my = bump(1)
                def spread(w16, m):
                    return [jnp.where(m, zero16, w16), jnp.where(m, w16, zero16)]
                yh, yl = split(wy)
                lhs = jnp.concatenate(spread(yh, my) + spread(yl, my), 0)
                lhs = jnp.concatenate([lhs, lhs], 1)
                hi, lo = [], []
                for ch in range(4):
                    a, b = split(row(5 + ch) * wx)
                    hi += spread(a, mx)
                    lo += spread(b, mx)
                rhs = jnp.concatenate([jnp.concatenate(hi, 0), jnp.concatenate(lo, 0)], 1)
                outs.append(lax.dot_general(lhs, rhs, (((1,), (1,)), ((), ())), preferred_element_type=jnp.float32))
            for u in range(UNR):
                t = jnp.where(own, tile_ref[0, first + g * UNR + u], mate_tile_ref[0, mate_first + g * UNR + u])
                out_ref[t] += outs[u][:32] + outs[u][32:]
            return c

        groups = lax.div(jnp.minimum(live_num, BLK) + (UNR - 1), UNR)
        lax.fori_loop(0, groups, one_group, 0)


def deposit_all(block_tile, block_count, corner, offset, radius, emission, extinction, tiles=512):
    mate_tile, mate_count, *mate_rest = share(block_tile, block_count, corner, offset, radius, emission, extinction)
    own_steps = KEPT // BLK
    steps = block_tile.shape[1] // BLK
    def own_at(i, tile, count, *unused):
        return jnp.minimum(jnp.minimum(i, own_steps - 1), lax.div(count[0, 0] - 1, BLK))
    def mate_at(i, *unused):
        return jnp.maximum(i - own_steps, 0)
    def specs(at):
        def m4(n):
            return pl.BlockSpec((n, 1, BLK, 128), lambda i, *scalars: (0, 0, at(i, *scalars), 0))
        def m3():
            return pl.BlockSpec((1, BLK, 128), lambda i, *scalars: (0, at(i, *scalars), 0))
        return [m4(2), m4(2), m3(), m4(3), m3()]
    return pl.pallas_call(
        functools.partial(deposit_kernel, own_steps),
        out_shape=pltpu.VMEM((tiles, 32, 128), jnp.float32),
        grid_spec=pltpu.PrefetchScalarGridSpec(
            num_scalar_prefetch=4, grid=(steps,),
            in_specs=specs(own_at) + specs(mate_at),
            out_specs=pl.BlockSpec((tiles, 32, 128), lambda i, *scalars: (0, 0, 0)),
            scratch_shapes=[pltpu.VMEM((9, BLK, 128), jnp.float32)],
        ),
        compiler_params=pltpu.CompilerParams(dimension_semantics=("arbitrary",), vmem_limit_bytes=56000 * 1024),
        name="deposit",
    )(block_tile, block_count, mate_tile, mate_count, corner, offset, radius, emission, extinction, *mate_rest)


def exchange_kernel(rank_ref, partial_ref, image_ref, order_ref, mine, pair, from_up, from_down, via_up, via_down, stack,
                    first_send, first_recv, pair_send, pair_recv, far_send, far_recv, near_send, near_recv, sum_send, sum_recv,
                    stack_send, stack_recv):
    d = lax.axis_index("depth")
    z = lax.axis_index("screen_0")
    core = lax.axis_index("screen_1")
    mate = 1 - core
    y, x = lax.div(d, 4), lax.rem(d, 4)
    z_up, z_down, z_far = lax.rem(z + 1, 4), lax.rem(z + 3, 4), lax.rem(z + 2, 4)
    turns = (2, 1, 3, 0)
    steps = (2, 3, 1, 0)
    summed_up = (2, 1)
    others = [(ry, rx) for ry in turns for rx in (2, 1, 3, 0) if (ry, rx) != (0, 0)]

    def away(ry, rx):
        return lax.rem(y + ry, 4) * 4 + lax.rem(x + rx, 4)

    def row(ry):
        return lax.rem(y + ry, 4) * 4

    barrier = pltpu.get_barrier_semaphore()
    pl.semaphore_signal(barrier, inc=1, device_id={"screen_1": mate}, device_id_type=MESH_ID)
    pl.semaphore_signal(barrier, inc=1, device_id={"screen_0": z_up}, device_id_type=MESH_ID)
    pl.semaphore_signal(barrier, inc=1, device_id={"screen_0": z_down}, device_id_type=MESH_ID)
    for ry, rx in others:
        pl.semaphore_signal(barrier, inc=1, device_id={"depth": away(ry, rx)}, device_id_type=MESH_ID)

    places = (z_far, z_up, z_down, z)

    def pair_copy(p, g):
        rows = pl.ds(row(g), 4)
        return pltpu.make_async_remote_copy(
            partial_ref.at[rows, places[p], mate], pair.at[rows, places[p]],
            pair_send.at[p, g], pair_recv.at[p, g], device_id={"screen_1": mate}, device_id_type=MESH_ID)

    def pair_far_copy(ry, rx):
        to = away(ry, rx)
        return pltpu.make_async_remote_copy(
            partial_ref.at[to, z_far, mate], pair.at[to, z_far],
            first_send.at[ry, rx], first_recv.at[ry, rx], device_id={"screen_1": mate}, device_id_type=MESH_ID)

    def line_copy(ry, rx, place, goal, to_up, send, recv):
        to, n = away(ry, rx), (2, 1, 3, 0).index(rx) % 2
        return pltpu.make_async_remote_copy(
            mine.at[to, place], goal.at[to], send.at[to_up, ry, n], recv.at[to_up, ry, n],
            device_id={"screen_0": z_up if to_up else z_down}, device_id_type=MESH_ID)

    def far_copy(ry, rx):
        to_up = int(rx in summed_up)
        return line_copy(ry, rx, z_far, via_up if to_up else via_down, to_up, far_send, far_recv)

    def near_copy(ry, rx):
        to_up = int(rx not in summed_up)
        return line_copy(ry, rx, z_up if to_up else z_down, from_up if to_up else from_down, to_up,
                         near_send, near_recv)

    def sum_copy(ry, rx):
        to_up = int(rx in summed_up)
        return line_copy(ry, rx, z_up if to_up else z_down, from_up if to_up else from_down, to_up,
                         sum_send, sum_recv)

    def stack_copy(ry, rx):
        to = away(ry, rx)
        return pltpu.make_async_remote_copy(
            mine.at[to, z], stack.at[d], stack_send.at[ry, rx], stack_recv.at[ry, rx],
            device_id={"depth": to}, device_id_type=MESH_ID)

    def add_in(first, num, place, terms):
        def one(i, c):
            total = terms[0](first + i)
            for term in terms[1:]:
                total = total + term(first + i)
            mine[first + i, place] = total
            return c
        lax.fori_loop(0, num, one, 0)

    pl.semaphore_wait(barrier, 18)
    for g in turns:
        for rx in steps:
            pair_far_copy(g, rx).start()
    for p in range(1, 4):
        for g in turns:
            pair_copy(p, g).start()

    for p in range(16):
        slab = 0
        for j in range(1, 16):
            slab = jnp.where(rank_ref[j] == p, j, slab)
        order_ref[p] = slab

    def take_pair(p, g):
        pair_copy(p, g).wait_recv()

    for g in turns:
        for rx in steps:
            pair_far_copy(g, rx).wait_recv()
            add_in(away(g, rx), 1, z_far, [lambda i: partial_ref[i, z_far, core], lambda i: pair[i, z_far]])
            far_copy(g, rx).start()
    for g in turns:
        for p, to_up in ((1, 1), (2, 0)):
            take_pair(p, g)
            add_in(row(g), 4, places[p], [
                lambda i, p=p: partial_ref[i, places[p], core], lambda i, p=p: pair[i, places[p]]])
            for rx in steps:
                if int(rx not in summed_up) == to_up:
                    near_copy(g, rx).start()
    for g in turns:
        for rx in steps:
            far_copy(g, rx).wait_recv()
            to_up = int(rx in summed_up)
            via, place = (via_up, z_up) if to_up else (via_down, z_down)
            add_in(away(g, rx), 1, place, [
                lambda i, place=place: mine[i, place], lambda i, via=via: via[i]])
            sum_copy(g, rx).start()
    for g in turns:
        take_pair(3, g)
        for rx in steps:
            near_copy(g, rx).wait_recv()
            sum_copy(g, rx).wait_recv()
            add_in(away(g, rx), 1, z, [
                lambda i: partial_ref[i, z, core], lambda i: pair[i, z], lambda i: from_up[i], lambda i: from_down[i]])
            if (g, rx) != (0, 0):
                stack_copy(g, rx).start()
    stack[d] = mine[d, z]
    for ry, rx in others:
        stack_copy(ry, rx).wait_recv()

    lane = lax.broadcasted_iota(jnp.int32, (2, 32, 128), 2)

    for t in (0, 2):
        def one_slab(p, carry, t=t):
            prior, light = carry
            value = stack[order_ref[p], pl.ds(t, 2)]
            own = jnp.where(lane >= 96, value, 0.0)
            twice = own + pltpu.roll(own, 32, 2)
            optical = twice + pltpu.roll(twice, 64, 2)
            light = light + jnp.exp(-(prior + 0.5 * optical)) * value
            return prior + optical, light
        zero = jnp.zeros((2, 32, 128), jnp.float32)
        prior, light = lax.fori_loop(0, 16, one_slab, (zero, zero), unroll=4)
        image_ref[pl.ds(t, 2)] = jnp.where(lane >= 96, 1.0 - jnp.exp(-prior), light)

    for g in turns:
        for p in range(1, 4):
            pair_copy(p, g).wait_send()
        for rx in steps:
            pair_far_copy(g, rx).wait_send()
            far_copy(g, rx).wait_send()
            near_copy(g, rx).wait_send()
            sum_copy(g, rx).wait_send()
    for ry, rx in others:
        stack_copy(ry, rx).wait_send()


def exchange(partial_value, slab_rank):
    dma = pltpu.SemaphoreType.DMA
    return pl.pallas_call(
        exchange_kernel,
        out_shape=jax.ShapeDtypeStruct((4, 32, 128), jnp.float32),
        in_specs=[pl.BlockSpec(memory_space=pltpu.SMEM), pl.BlockSpec(memory_space=pltpu.VMEM)],
        out_specs=pl.BlockSpec(memory_space=pltpu.VMEM),
        scratch_shapes=[
            pltpu.SMEM((16,), jnp.int32),
            pltpu.VMEM((16, 4, 4, 32, 128), jnp.float32),
            pltpu.VMEM((16, 4, 4, 32, 128), jnp.float32),
            pltpu.VMEM((16, 4, 32, 128), jnp.float32),
            pltpu.VMEM((16, 4, 32, 128), jnp.float32),
            pltpu.VMEM((16, 4, 32, 128), jnp.float32),
            pltpu.VMEM((16, 4, 32, 128), jnp.float32),
            pltpu.VMEM((16, 4, 32, 128), jnp.float32),
            dma((4, 4)), dma((4, 4)), dma((4, 4)), dma((4, 4)),
            *[dma((2, 4, 2))] * 6,
            dma((4, 4)), dma((4, 4)),
        ],
        compiler_params=pltpu.CompilerParams(collective_id=0, has_side_effects=True, vmem_limit_bytes=24 * 2**20),
        name="exchange",
    )(slab_rank, partial_value.reshape(16, 4, 2, 4, 32, 128))


def shards(block_tile, block_count, slab_rank, corner, offset, radius, emission, extinction):
    partial_value = deposit_all(
        block_tile, block_count, corner, offset, radius, emission, extinction
    )
    return exchange(partial_value, slab_rank)


def solution(mesh):
    torus = Mesh(mesh.devices.reshape(mesh.shape["depth"], 4, 2), ("depth", "screen_0", "screen_1"))
    placed = (
        P("depth", SCREEN),
        P("depth", SCREEN),
        P(),
        P(None, "depth", SCREEN, None),
        P(None, "depth", SCREEN, None),
        P("depth", SCREEN, None),
        P(None, "depth", SCREEN, None),
        P("depth", SCREEN, None),
    )
    return jax.shard_map(
        shards, mesh=torus, in_specs=placed, out_specs=P(DEPTH_SCREEN, None, None), check_vma=False
    )
```
